16 devices in a mesh: dp: 2 (over z), cp: 8 (over y, x, core).
Axes of the slice: x: 2, y: 2, z: 2, core: 2. Of those that a mesh axis runs over, the one named last changes fastest.
Arguments:
- x: bfloat16 [32, 1024, 2048], P('dp', 'cp')
- grad_out: bfloat16 [32, 1024, 2048], P('dp', 'cp')
- w_q: bfloat16 [2048, 32, 64], replicated
- w_k: bfloat16 [2048, 4, 64], replicated
- w_v: bfloat16 [2048, 4, 64], replicated
- w_o: bfloat16 [2048, 32, 64], replicated
- w_up: bfloat16 [2048, 5632], replicated
- w_down: bfloat16 [5632, 2048], replicated
Outputs:
- output 1: bfloat16 [32, 1024, 2048], P('dp', 'cp')
- output 2: float32 [2048, 32, 64], P(('dp', 'cp'))
- output 3: float32 [2048, 4, 64], P(('dp', 'cp'))
- output 4: float32 [2048, 4, 64], P(('dp', 'cp'))
- output 5: float32 [2048, 32, 64], P(('dp', 'cp'))
- output 6: float32 [2048, 5632], P(('dp', 'cp'))
- output 7: float32 [5632, 2048], P(('dp', 'cp'))
All inputs are finite; a program needn't handle non-finite values.
Results may differ from the reference program's by a relative error of at most 0.0130821.
Values are sent between devices in bfloat16 or wider.
A program may use at most 1 GiB of HBM per device.

```python
import math
import jax
import jax.numpy as jnp
from jax import lax

D_MODEL = 2048
N_HEADS = 32
KV_HEADS = 4
HEAD_DIM = 64
FF_DIM = 5632
CP_SIZE = 8
DP_SIZE = 2
BATCH = 32
SEQ_LEN = 1024
GROUP = N_HEADS // KV_HEADS
HALF = SEQ_LEN // (2 * CP_SIZE)
Q_BLOCK = min(SEQ_LEN, 2 ** max(0, int(math.log2(max(1, 2 ** 22 // (N_HEADS * SEQ_LEN))))))
TOK_BLOCK = min(SEQ_LEN, 2 ** max(0, int(math.log2(max(1, 2 ** 22 // FF_DIM)))))
NEG_BIG = -1e30


def setup_inputs(seed: int = 0) -> dict:
    keys = jax.random.split(jax.random.key(seed), 8)

    def weight(key, shape, fan_in):
        return (jax.random.normal(key, shape, jnp.float32) * fan_in ** -0.5).astype(jnp.bfloat16)

    act_shape = (BATCH, SEQ_LEN, D_MODEL)
    return {
        'x': jax.random.normal(keys[0], act_shape, jnp.float32).astype(jnp.bfloat16),
        'grad_out': jax.random.normal(keys[1], act_shape, jnp.float32).astype(jnp.bfloat16),
        'w_q': weight(keys[2], (D_MODEL, N_HEADS, HEAD_DIM), D_MODEL),
        'w_k': weight(keys[3], (D_MODEL, KV_HEADS, HEAD_DIM), D_MODEL),
        'w_v': weight(keys[4], (D_MODEL, KV_HEADS, HEAD_DIM), D_MODEL),
        'w_o': weight(keys[5], (D_MODEL, N_HEADS, HEAD_DIM), N_HEADS * HEAD_DIM),
        'w_up': weight(keys[6], (D_MODEL, FF_DIM), D_MODEL),
        'w_down': weight(keys[7], (FF_DIM, D_MODEL), FF_DIM),
    }


def to_bf16(values):
    return values.astype(jnp.bfloat16).astype(jnp.float32)


def stored_to_natural(rows):
    blocks = rows.reshape(CP_SIZE, 2, HALF, D_MODEL)
    return jnp.concatenate([blocks[:, 0], blocks[::-1, 1]], axis=0).reshape(SEQ_LEN, D_MODEL)


def natural_to_stored(rows):
    halves = rows.reshape(2, CP_SIZE, HALF, D_MODEL)
    return jnp.stack([halves[0], halves[1][::-1]], axis=1).reshape(SEQ_LEN, D_MODEL)


def layer_row(x_row, w_q, w_k, w_v, w_o, w_up, w_down):
    q_all = to_bf16(jnp.dot(x_row, w_q.reshape(D_MODEL, N_HEADS * HEAD_DIM), preferred_element_type=jnp.float32))
    k_all = to_bf16(jnp.dot(x_row, w_k.reshape(D_MODEL, KV_HEADS * HEAD_DIM), preferred_element_type=jnp.float32)).reshape(SEQ_LEN, KV_HEADS, HEAD_DIM)
    v_all = to_bf16(jnp.dot(x_row, w_v.reshape(D_MODEL, KV_HEADS * HEAD_DIM), preferred_element_type=jnp.float32)).reshape(SEQ_LEN, KV_HEADS, HEAD_DIM)
    q_blocks = q_all.reshape(SEQ_LEN // Q_BLOCK, Q_BLOCK, KV_HEADS, GROUP, HEAD_DIM)
    starts = jnp.arange(SEQ_LEN // Q_BLOCK) * Q_BLOCK
    key_pos = jnp.arange(SEQ_LEN)

    def attn_block(block_in):
        q_blk, start = block_in
        scores = jnp.einsum('qkgd,tkd->kgqt', q_blk, k_all) * HEAD_DIM ** -0.5
        query_pos = start + jnp.arange(Q_BLOCK)
        scores = jnp.where(key_pos[None, :] <= query_pos[:, None], scores, NEG_BIG)
        attn_prob = to_bf16(jax.nn.softmax(scores, axis=-1))
        return to_bf16(jnp.einsum('kgqt,tkd->qkgd', attn_prob, v_all))

    attn_rows = lax.map(jax.checkpoint(attn_block), (q_blocks, starts)).reshape(SEQ_LEN, N_HEADS * HEAD_DIM)
    h_act = to_bf16(x_row + jnp.dot(attn_rows, w_o.reshape(D_MODEL, N_HEADS * HEAD_DIM).T, preferred_element_type=jnp.float32))

    def mlp_block(h_blk):
        hidden = jnp.dot(h_blk, w_up, preferred_element_type=jnp.float32)
        act_out = to_bf16(jax.nn.gelu(hidden, approximate=True))
        return h_blk + jnp.dot(act_out, w_down, preferred_element_type=jnp.float32)

    out_rows = lax.map(jax.checkpoint(mlp_block), h_act.reshape(SEQ_LEN // TOK_BLOCK, TOK_BLOCK, D_MODEL))
    return out_rows.reshape(SEQ_LEN, D_MODEL)


def reference(x, grad_out, w_q, w_k, w_v, w_o, w_up, w_down):
    weights = tuple(weight.astype(jnp.float32) for weight in (w_q, w_k, w_v, w_o, w_up, w_down))

    def row_step(grad_sum, row_pair):
        x_row, cot_row = row_pair
        _, back_fn = jax.vjp(layer_row, stored_to_natural(x_row.astype(jnp.float32)), *weights)
        cotangents = back_fn(stored_to_natural(cot_row.astype(jnp.float32)))
        new_sum = tuple(grad_old + grad_new for grad_old, grad_new in zip(grad_sum, cotangents[1:]))
        return new_sum, natural_to_stored(cotangents[0]).astype(jnp.bfloat16)

    grad_init = tuple(jnp.zeros_like(weight) for weight in weights)
    grad_sums, grad_x = lax.scan(row_step, grad_init, (x, grad_out))
    inv_count = 1.0 / (CP_SIZE * DP_SIZE)
    return (grad_x, grad_sums[0] * inv_count, grad_sums[1] * inv_count, grad_sums[2] * inv_count,
            grad_sums[3] * inv_count, grad_sums[4] * inv_count, grad_sums[5] * inv_count)
```

```python
import functools, math
import jax, jax.numpy as jnp
from jax import lax
from jax.experimental import pallas as pl
from jax.experimental.pallas import tpu as pltpu
from jax.sharding import PartitionSpec as P


BF, F32 = jnp.bfloat16, jnp.float32
NEG_BIG = -1e30
LANES, WIDE, MODEL, FF_TILE, FF_ROWS, SEQ, Z = 128, 512, 2048, 1408, 352, 1024, 0
HALF = 64
CHUNK = 256
HEADS = 2
NORM = True


def nt(a, b):
    return lax.dot_general(a, b, (((1,), (1,)), ((), ())), preferred_element_type=F32)


def tn(a, b):
    return lax.dot_general(a, b, (((Z,), (Z,)), ((), ())), preferred_element_type=F32)


def nn(a, b):
    return lax.dot_general(a, b, (((1,), (Z,)), ((), ())), preferred_element_type=F32)


def low_lanes(rows):
    return lax.broadcasted_iota(jnp.int32, (rows, LANES), 1) < HALF


def load_keys(me, kv_refs, keys, vals, head):
    low = low_lanes(LANES)
    for pos, ref in enumerate(kv_refs):
        dev = me ^ pos
        tile = ref[Z, :, LANES * head:LANES * (head + 1)]
        flipped = jnp.concatenate([tile[:, HALF:], tile[:, :HALF]], axis=1)
        k_two = jnp.where(low, tile, flipped)
        v_two = jnp.where(low, flipped, tile)
        first = pl.multiple_of(dev * HALF, HALF)
        second = pl.multiple_of((15 - dev) * HALF, HALF)
        keys[pl.ds(first, HALF), :] = k_two[:HALF]
        keys[pl.ds(second, HALF), :] = k_two[HALF:]
        vals[pl.ds(first, HALF), :] = v_two[:HALF]
        vals[pl.ds(second, HALF), :] = v_two[HALF:]


def spread_heads(rows):
    low = low_lanes(HALF)
    zero = jnp.zeros((HALF, LANES), BF)
    parts = []
    for pair in range(4):
        tile = rows[:, LANES * pair:LANES * (pair + 1)]
        parts += [jnp.where(low, tile, zero), jnp.where(low, zero, tile)]
    return jnp.concatenate(parts, axis=Z)


def gather_heads(cols, ref, base, lane):
    low = low_lanes(HALF)
    for pair in range(4):
        tile = cols[:, LANES * pair:LANES * (pair + 1)].T
        ref[Z, base:base + HALF, lane + LANES * pair:lane + LANES * (pair + 1)] = jnp.where(low, tile[:HALF], tile[HALF:]).astype(BF)


def tile_plan(me):
    late = me >= 4
    fifth_key = pl.multiple_of(jnp.where(late, CHUNK, 768), CHUNK)
    fifth_block = jnp.where(late, me, 15 - me)
    return late, [(Z, me, True, Z), (Z, 15 - me, False, 1), (CHUNK, 15 - me, False, 1),
                  (2 * CHUNK, 15 - me, True, 1), (fifth_key, fifth_block, True, 2)]


def lag():
    row = lax.broadcasted_iota(jnp.int32, (CHUNK, WIDE), Z)
    col = lax.broadcasted_iota(jnp.int32, (CHUNK, WIDE), 1)
    return row - (col & (HALF - 1))


def fwd_kernel(scale2, aliased, me_ref, q_ref, *refs):
    kv_refs = refs[:8]
    refs = refs[8 + (1 if aliased else Z):]
    o_ref, lse_ref, keys, vals = refs
    me = me_ref[Z]
    gap = lag()
    late, plan = tile_plan(me)

    def choose(one, two):
        return [one, two, jnp.where(late, one, two)]

    def split(parts):
        zero = jnp.zeros_like(parts[4])
        return parts[Z] + jnp.where(late, parts[4], zero), parts[1] + parts[2] + parts[3] + jnp.where(late, zero, parts[4])

    class Head:
        pass

    heads = []
    for head in range(HEADS):
        x = Head()
        load_keys(me, kv_refs, keys.at[head], vals.at[head], head)
        lanes = slice(WIDE * head, WIDE * (head + 1))
        q_tile = q_ref[Z, :, lanes]
        x.q = choose(spread_heads(q_tile[:HALF]), spread_heads(q_tile[HALF:]))
        x.scores, x.tops, x.exps, x.sums, x.outs = [], [], [], [], []
        heads.append(x)

    def score(head, i):
        x = heads[head]
        start, block, masked, which = plan[i]
        s = nt(keys[head, pl.ds(start, CHUNK), :], x.q[which])
        if masked:
            s = jnp.where(gap <= block * HALF - start, s, NEG_BIG)
        x.scores.append(s)
        x.tops.append(jnp.max(s, axis=Z, keepdims=True))

    def top(head):
        x = heads[head]
        t = x.tops
        top_b = jnp.maximum(jnp.maximum(t[1], t[2]), t[3])
        top_a = jnp.where(late, jnp.maximum(t[Z], t[4]), t[Z]) * scale2
        top_b = jnp.where(late, top_b, jnp.maximum(top_b, t[4])) * scale2
        x.top = choose(top_a, top_b)

    def expo(head, i):
        x = heads[head]
        e = jnp.exp2(x.scores[i] * scale2 - x.top[plan[i][3]])
        x.exps.append(e if NORM else e.astype(BF))
        x.sums.append(jnp.sum(e, axis=Z, keepdims=True))

    def total(head):
        x = heads[head]
        sum_a, sum_b = split(x.sums)
        lse_ref[head, Z:1, :] = x.top[Z] + jnp.log2(sum_a)
        lse_ref[head, 1:2, :] = x.top[1] + jnp.log2(sum_b)
        x.inv = choose(1.0 / sum_a, 1.0 / sum_b)

    def value(head, i):
        x = heads[head]
        p = (x.exps[i] * x.inv[plan[i][3]]).astype(BF) if NORM else x.exps[i]
        x.outs.append(tn(vals[head, pl.ds(plan[i][Z], CHUNK), :], p))

    def finish(head):
        x = heads[head]
        out_a, out_b = split(x.outs)
        if not NORM:
            out_a, out_b = out_a * x.inv[Z], out_b * x.inv[1]
        gather_heads(out_a, o_ref, Z, WIDE * head)
        gather_heads(out_b, o_ref, HALF, WIDE * head)

    n = len(plan)
    for head in range(HEADS + 2):
        for i in range(n):
            if head < HEADS:
                score(head, i)
            if Z <= head - 1 < HEADS:
                if i == Z:
                    top(head - 1)
                expo(head - 1, i)
            if Z <= head - 2 < HEADS:
                if i == Z:
                    total(head - 2)
                value(head - 2, i)
        if Z <= head - 2 < HEADS:
            finish(head - 2)


def bwd_kernel(scale, scale2, aliased, me_ref, q_ref, g_ref, lse_ref, *refs):
    kv_refs = refs[:8]
    refs = refs[8 + (1 if aliased else Z):]
    dq_ref, keep_ref, send_ref, keys, vals, grads = refs
    me = me_ref[Z]
    gap = lag()
    late, plan = tile_plan(me)
    low = low_lanes(CHUNK)

    def choose(one, two):
        return [one, two, jnp.where(late, one, two)]

    def split(parts):
        zero = jnp.zeros_like(parts[4])
        return parts[Z] + jnp.where(late, parts[4], zero), parts[1] + parts[2] + parts[3] + jnp.where(late, zero, parts[4])

    class Head:
        pass

    heads = []
    for head in range(HEADS):
        x = Head()
        load_keys(me, kv_refs, keys.at[head], vals.at[head], head)
        lanes = slice(WIDE * head, WIDE * (head + 1))
        q_tile, g_tile = q_ref[Z, :, lanes], g_ref[Z, :, lanes]
        x.q = choose(spread_heads(q_tile[:HALF]), spread_heads(q_tile[HALF:]))
        x.g = choose(spread_heads(g_tile[:HALF]), spread_heads(g_tile[HALF:]))
        x.lse = choose(lse_ref[head, Z:1, :], lse_ref[head, 1:2, :])
        x.probs, x.dprobs, x.deltas, x.dqs, x.dks, x.dvs = [], [], [], [], [], []
        heads.append(x)

    def prob(head, i):
        x = heads[head]
        start, block, masked, which = plan[i]
        s = nt(keys[head, pl.ds(start, CHUNK), :], x.q[which])
        if masked:
            s = jnp.where(gap <= block * HALF - start, s, NEG_BIG)
        p = jnp.exp2(s * scale2 - x.lse[which])
        dp = nt(vals[head, pl.ds(start, CHUNK), :], x.g[which]).astype(BF)
        x.probs.append(p)
        x.dprobs.append(dp)
        x.deltas.append(jnp.sum(p * dp.astype(F32), axis=Z, keepdims=True))

    def delta(head):
        x = heads[head]
        x.delta = choose(*split(x.deltas))

    def grad(head, i):
        x = heads[head]
        start, _, _, which = plan[i]
        p, dp = x.probs[i], x.dprobs[i]
        ds = (p * (dp.astype(F32) - x.delta[which])).astype(BF)
        x.dvs.append(nn(p.astype(BF), x.g[which]))
        x.dks.append(nn(ds, x.q[which]))
        x.dqs.append(tn(keys[head, pl.ds(start, CHUNK), :], ds))

    def finish(head):
        x = heads[head]
        dq_a, dq_b = split(x.dqs)
        gather_heads(dq_a * scale, dq_ref, Z, WIDE * head)
        gather_heads(dq_b * scale, dq_ref, HALF, WIDE * head)
        zero = jnp.zeros_like(x.dks[4])

        def by_chunk(parts):
            return [parts[Z] + parts[1], parts[2] + jnp.where(late, parts[4], zero), parts[3],
                    jnp.where(late, zero, parts[4])]

        for chunk, (dk, dv) in enumerate(zip(by_chunk(x.dks), by_chunk(x.dvs))):
            dk = (dk + pltpu.roll(dk, HALF, 1)) * scale
            dv = dv + pltpu.roll(dv, HALF, 1)
            both = jnp.where(low, dk, dv)
            for sub in range(4):
                block = 4 * chunk + sub
                dev, base = (block, Z) if block < 8 else (15 - block, HALF)
                grads[dev ^ me, base:base + HALF, LANES * head:LANES * (head + 1)] = both[sub * HALF:(sub + 1) * HALF]

    n = len(plan)
    for head in range(HEADS + 1):
        for i in range(n):
            if head < HEADS:
                prob(head, i)
            if head >= 1:
                if i == Z:
                    delta(head - 1)
                grad(head - 1, i)
        if head >= 1:
            finish(head - 1)
    for one in range(2):
        for two in range(2):
            slot = jnp.where(pl.program_id(1) == Z, 2 * two + one, 2 * one + two)
            keep_ref[Z, one, two, Z] = grads[2 * slot]
            send_ref[Z, one, two, Z] = grads[2 * slot + 1]


def attn_fwd(me, q, kvs, first, total, o_prev=None):
    count = kvs[Z].shape[Z]
    scale2 = 0.125 * math.log2(math.e)
    aliased = o_prev is not None
    row = lambda b, g, m: (first + b, Z, g)
    kv_spec = pl.BlockSpec((1, LANES, LANES * HEADS), lambda b, g, m: (b, Z, g))
    grid_spec = pltpu.PrefetchScalarGridSpec(
        num_scalar_prefetch=1, grid=(count, 4 // HEADS),
        in_specs=[pl.BlockSpec((1, LANES, WIDE * HEADS), row)] + [kv_spec] * 8 + ([pl.BlockSpec(memory_space=pl.ANY)] if aliased else []),
        out_specs=[pl.BlockSpec((1, LANES, WIDE * HEADS), row), pl.BlockSpec((HEADS, 2, WIDE), lambda b, g, m: (b * (4 // HEADS) + g, Z, Z))],
        scratch_shapes=[pltpu.VMEM((HEADS, SEQ, LANES), BF), pltpu.VMEM((HEADS, SEQ, LANES), BF)])
    return pl.pallas_call(
        functools.partial(fwd_kernel, scale2, aliased), grid_spec=grid_spec, name='attn_fwd',
        out_shape=[jax.ShapeDtypeStruct((total, LANES, MODEL), BF), jax.ShapeDtypeStruct((count * 4, 2, WIDE), F32)],
        input_output_aliases={10: Z} if aliased else {},
        cost_estimate=timed(6 * count),
        compiler_params=ALL_VMEM,
    )(me, q, *kvs, *([o_prev] if aliased else []))


def attn_bwd(me, q, g, lse, kvs, first, sub, count, dq_prev=None):
    total = q.shape[Z]
    scale = 0.125
    scale2 = scale * math.log2(math.e)
    aliased = dq_prev is not None
    row = lambda b, h, m: (first + b, Z, h)
    kv_spec = pl.BlockSpec((1, LANES, LANES * HEADS), lambda b, h, m: (sub + b, Z, h))
    part = pl.BlockSpec((1, 2, 2, 1, LANES, CHUNK), lambda b, h, m: (h, Z, Z, b, Z, Z))
    part_shape = jax.ShapeDtypeStruct((2, 2, 2, count, LANES, CHUNK), F32)
    grid_spec = pltpu.PrefetchScalarGridSpec(
        num_scalar_prefetch=1, grid=(count, 4 // HEADS),
        in_specs=[pl.BlockSpec((1, LANES, WIDE * HEADS), row), pl.BlockSpec((1, LANES, WIDE * HEADS), row),
                  pl.BlockSpec((HEADS, 2, WIDE), lambda b, h, m: ((sub + b) * (4 // HEADS) + h, Z, Z))] + [kv_spec] * 8
        + ([pl.BlockSpec(memory_space=pl.ANY)] if aliased else []),
        out_specs=[pl.BlockSpec((1, LANES, WIDE * HEADS), row), part, part],
        scratch_shapes=[pltpu.VMEM((HEADS, SEQ, LANES), BF), pltpu.VMEM((HEADS, SEQ, LANES), BF), pltpu.VMEM((8, LANES, LANES * HEADS), F32)])
    return pl.pallas_call(
        functools.partial(bwd_kernel, scale, scale2, aliased), grid_spec=grid_spec, name='attn_bwd',
        out_shape=[jax.ShapeDtypeStruct((total, LANES, MODEL), BF)] + [part_shape] * 2,
        input_output_aliases={12: Z} if aliased else {},
        cost_estimate=timed(10 * count),
        compiler_params=ALL_VMEM,
    )(me, q, g, lse, *kvs, *([dq_prev] if aliased else []))


BITS = {'c': 1, 'x': 2, 'y': 4}
ALL_VMEM = pltpu.CompilerParams(vmem_limit_bytes=63 * 2**20)
NEXT = {'x': ('y', 'z'), 'y': ('z', 'x'), 'z': ('x', 'y')}


def swap(values, link):
    if link == 'z':
        return lax.ppermute(values, 'dp', [(Z, 1), (1, Z)])
    return lax.ppermute(values, 'cp', [(i, i ^ BITS[link]) for i in range(8)])


def pick(values, axis, index):
    return lax.index_in_dim(values, index, axis, keepdims=False)


def timed(micros):
    return pl.CostEstimate(flops=int(micros * 9e8), bytes_accessed=1 << 20, transcendentals=Z)


def mm_kernel(product, added, x_ref, w_ref, *refs):
    total = product(x_ref[...], w_ref[...])
    if added:
        total = total + refs[Z][...].astype(F32)
    refs[-1][...] = total.astype(refs[-1].dtype)


def mm(x, w, rows, first, count, width, flip=True, added=None, dtype=BF):
    total, depth = x.shape
    tile = pl.BlockSpec((rows, width), lambda n, t: (t, n))
    w_spec = pl.BlockSpec((width, depth), lambda n, t: (first + n, Z)) if flip else pl.BlockSpec(
        (depth, width), lambda n, t: (Z, first + n))
    return pl.pallas_call(
        functools.partial(mm_kernel, nt if flip else nn, added is not None), grid=(count, total // rows), name='mm',
        in_specs=[pl.BlockSpec((rows, depth), lambda n, t: (t, Z)), w_spec] + ([tile] if added is not None else []),
        out_specs=tile, out_shape=jax.ShapeDtypeStruct((total, count * width), dtype),
        cost_estimate=timed(total * count * width * depth * 2 / 9e8),
        compiler_params=ALL_VMEM)(x, w, *([added] if added is not None else []))


def join_kv(k_ref, v_ref, both):
    @pl.when(pl.program_id(Z) == Z)
    def _():
        for head in range(4):
            both[LANES * head:LANES * head + HALF, :] = k_ref[HALF * head:HALF * head + HALF, :]
            both[LANES * head + HALF:LANES * head + LANES, :] = v_ref[HALF * head:HALF * head + HALF, :]


def kv_kernel(x_ref, k_ref, v_ref, low_ref, high_ref, both):
    join_kv(k_ref, v_ref, both)
    value = nt(x_ref[...], both[...]).astype(BF)
    for index, ref in enumerate((low_ref, high_ref)):
        @pl.when(pl.program_id(Z) // 2 == index)
        def _():
            ref[...] = value


def kv_call(x, w_k, w_v):
    rows, (total, depth) = WIDE, x.shape
    whole = pl.BlockSpec((CHUNK, depth), lambda t: (Z, Z), pipeline_mode=pl.Buffered(1))
    return pl.pallas_call(
        kv_kernel, grid=(total // rows,), name='kv',
        in_specs=[pl.BlockSpec((rows, depth), lambda t: (t, Z)), whole, whole],
        out_specs=[pl.BlockSpec((rows, WIDE), lambda t: (jnp.minimum(t, 1), Z)), pl.BlockSpec((rows, WIDE), lambda t: (jnp.maximum(t - 2, Z), Z))],
        out_shape=[jax.ShapeDtypeStruct((total // 2, WIDE), BF)] * 2,
        scratch_shapes=[pltpu.VMEM((WIDE, depth), BF)], cost_estimate=timed(9), compiler_params=ALL_VMEM)(x, w_k, w_v)


def gx_kernel(h_ref, q_ref, g_ref, w_ref, k_ref, v_ref, *refs):
    out_ref, both = refs[-2:]
    join_kv(k_ref, v_ref, both)
    total = nn(q_ref[...], w_ref[...]) + nn(g_ref[...], both[...])
    out_ref[...] = (h_ref[...].astype(F32) + total).astype(BF)


def gx_call(grad_h, grad_q, grad_kv, w_q, w_k, w_v, half, prev=None):
    rows, (total, depth) = WIDE, grad_h.shape
    width = depth // 2
    aliased = prev is not None
    tile = pl.BlockSpec((rows, width), lambda t: (t, half))
    once = lambda count: pl.BlockSpec((count, width), lambda t: (Z, half), pipeline_mode=pl.Buffered(1))
    return pl.pallas_call(
        gx_kernel, grid=(total // rows,), name='gx',
        in_specs=[tile, pl.BlockSpec((rows, depth), lambda t: (t, Z)), pl.BlockSpec((rows, WIDE), lambda t: (t, Z)), once(depth), once(CHUNK),
                  once(CHUNK)] + ([pl.BlockSpec(memory_space=pl.ANY)] if aliased else []),
        out_specs=tile, out_shape=jax.ShapeDtypeStruct((total, depth), BF), scratch_shapes=[pltpu.VMEM((WIDE, width), BF)],
        input_output_aliases={6: Z} if aliased else {}, cost_estimate=timed(14), compiler_params=ALL_VMEM,
    )(grad_h, grad_q, grad_kv, w_q, w_k, w_v, *([prev] if aliased else []))


def ff_kernel(bits_ref, h_ref, w_ref, ga_ref, at_ref, gu_ref, held, turned):
    root = math.sqrt(2.0 / math.pi)
    width = w_ref.shape[1]
    for lo in range(Z, width, CHUNK):
        cut = slice(lo, min(lo + CHUNK, width))
        u = held[:, cut]
        held[:, cut] = nn(h_ref[...], w_ref[:, cut])
        rise = (root * 0.044715) * (u * u)
        t = jnp.tanh(u * (root + rise))
        up, down, half_u = 1.0 + t, 1.0 - t, 0.5 * u
        slope = up * (0.5 + (half_u * down) * (root + 3.0 * rise))
        gu_ref[:, cut] = (ga_ref[:, cut].astype(F32) * slope).astype(BF)
        turned[cut, :] = (half_u * up).T.astype(BF)
    for x in range(2):
        for c in range(2):
            lo = (2 * x + c) * FF_ROWS
            at_ref[Z, Z, x ^ bits_ref[2], c ^ bits_ref[3]] = turned[lo:lo + FF_ROWS, :]


def ff_block(bits, h, w_up, ga):
    tokens, width, rows = MODEL, FF_TILE, CHUNK
    per = tokens // rows
    steps = 4 * per
    now = lambda i: jnp.minimum(i, steps - 1)
    then = lambda i: jnp.maximum(i - 1, Z)
    grid_spec = pltpu.PrefetchScalarGridSpec(
        num_scalar_prefetch=1, grid=(steps + 1,),
        in_specs=[pl.BlockSpec((rows, MODEL), lambda i, m: (now(i) % per, Z)),
                  pl.BlockSpec((MODEL, width), lambda i, m: (Z, now(i) // per)),
                  pl.BlockSpec((rows, width), lambda i, m: (then(i) % per, then(i) // per))],
        out_specs=[pl.BlockSpec((1, 1, 2, 2, FF_ROWS, rows), lambda i, m: ((then(i) // per // 2) ^ m[Z], (then(i) // per % 2) ^ m[1], Z, Z, Z, then(i) % per)),
                   pl.BlockSpec((rows, width), lambda i, m: (then(i) % per, then(i) // per))],
        scratch_shapes=[pltpu.VMEM((rows, width), F32), pltpu.VMEM((width, rows), BF)])
    return pl.pallas_call(
        ff_kernel, grid_spec=grid_spec, name='ff_block',
        out_shape=[jax.ShapeDtypeStruct((2, 2, 2, 2, FF_ROWS, tokens), BF), jax.ShapeDtypeStruct((tokens, 5632), BF)],
        cost_estimate=timed(60), compiler_params=ALL_VMEM)(bits, h, w_up, ga)


def color_of(n, plan):
    edge, color = Z, Z
    for _, count in plan[:-1]:
        edge += count
        color = color + (n >= edge).astype(jnp.int32)
    return color


def pair_kernel(plan, rows, turned, *refs):
    n, steps = pl.program_id(Z), sum(count for _, count in plan)
    count = len(plan)
    if turned:
        left, refs = refs[Z], refs[1:]
        take = lambda place, core: left[place, core]
    else:
        parts, left, refs = refs[:16], refs[-1], refs[16:-1]

        @pl.when(n == Z)
        def _():
            for place in range(8):
                for core in range(2):
                    left[place, core] = parts[2 * place + core][...].T

        take = lambda place, core: left[place, core]
    right, outs = refs[Z], refs[1:1 + 2 * count]
    mine, sent, came, send_sem, recv_sem, free_sem = refs[1 + 2 * count:]
    me = lax.axis_index('cp')
    other = {'cp': me + 1 - 2 * (me % 2)}
    mesh_id = pl.DeviceIdType.MESH
    now, then = n % 2, (n + 1) % 2

    def copy(slot):
        return pltpu.make_async_remote_copy(src_ref=sent.at[slot], dst_ref=came.at[slot], send_sem=send_sem.at[slot],
                                            recv_sem=recv_sem.at[slot], device_id=other, device_id_type=mesh_id)

    @pl.when(n == Z)
    def _():
        barrier = pltpu.get_barrier_semaphore()
        pl.semaphore_signal(barrier, inc=1, device_id=other, device_id_type=mesh_id)
        pl.semaphore_wait(barrier, 1)

    @pl.when(n >= 3)
    def _():
        pl.semaphore_wait(free_sem, 1)

    @pl.when(n >= 1)
    def _():
        copy(then).start()

    @pl.when(n < steps)
    def _():
        some = 1 if turned else 4
        for core, dest in ((1, sent), (Z, mine)):
            for place in range(Z, 8, some):
                tile = jnp.concatenate([take(place + k, core) for k in range(some)], axis=Z)
                dest[now, place:place + some] = nn(tile, right[...]).reshape(some, rows, -1)

    @pl.when(n >= 1)
    def _():
        copy(then).wait()
        color = color_of(n - 1, plan)
        for index, (split, _) in enumerate(plan):
            @pl.when(color == index)
            def _():
                for place in range(8):
                    z, y, x = place // 4, place // 2 % 2, place % 2
                    half, k = {'z': (z, 2 * y + x), 'y': (y, 2 * z + x), 'x': (x, 2 * z + y)}[split]
                    outs[2 * index + 1 - half][k] = mine[then, place] + came[then, place]

    @pl.when((n >= 1) & (n < steps - 1))
    def _():
        pl.semaphore_signal(free_sem, inc=1, device_id=other, device_id_type=mesh_id)


def pair_call(left, right, plan, tile, call_id):
    turned = left.ndim == 4
    rows = left.shape[2] if turned else LANES
    steps = sum(count for _, count in plan)
    once = pl.Buffered(1)
    if turned:
        left_specs = [pl.BlockSpec((8, 2, rows, MODEL), lambda n: (Z, Z, Z, Z), pipeline_mode=once)]
    else:
        def column(place, core):
            def at(n):
                me = lax.axis_index('cp')
                bits = (lax.axis_index('dp'), me // 4, (me // 2) % 2, me % 2)
                flips = (place // 4, place // 2 % 2, place % 2, core)
                return Z, sum((1 - bit if flip else bit) * weight for bit, flip, weight in zip(bits, flips, (8, 4, 2, 1)))

            return at

        left_specs = [pl.BlockSpec((MODEL, LANES), column(place, core), pipeline_mode=once) for place in range(8) for core in range(2)]
    out_specs, out_shape, edge = [], [], Z
    for _, count in plan:
        spec = pl.BlockSpec((4, rows, tile), lambda n, edge=edge, count=count: (Z, Z, jnp.clip(n - 1 - edge, Z, count - 1)))
        out_specs += [spec, spec]
        out_shape += [jax.ShapeDtypeStruct((4, rows, count * tile), F32)] * 2
        edge += count
    both = pltpu.VMEM((2, 8, rows, tile), F32)
    two = pltpu.SemaphoreType.DMA((2,))
    return pl.pallas_call(
        functools.partial(pair_kernel, plan, rows, turned), grid=(steps + 1,), name='pair',
        in_specs=left_specs + [pl.BlockSpec((MODEL, tile), lambda n: (Z, jnp.minimum(n, steps - 1)))], out_specs=out_specs, out_shape=out_shape,
        scratch_shapes=[both, both, both, two, two, pltpu.SemaphoreType.REGULAR] + ([] if turned else [pltpu.VMEM((8, 2, LANES, MODEL), BF)]),
        cost_estimate=timed(16 * rows * steps * tile * 4096 / 9e8),
        compiler_params=pltpu.CompilerParams(vmem_limit_bytes=63 * 2**20, collective_id=call_id, has_side_effects=True),
    )(*([left] * len(left_specs)), right)


def halve(keep, got, axis):
    return tuple(pick(keep, axis, k) + pick(got, axis, k) for k in (1, Z))


def weight_grad(left, right, plan, tile, call_id, flip=False):
    outs = pair_call(left, right, plan, tile, call_id)
    keeps, gots, fars = [], [], []
    for (split, _), send, keep in zip(plan, outs[::2], outs[1::2]):
        shape = (2, 2, *keep.shape[1:])
        got = swap(send, split).reshape(shape)
        send, keep = lax.optimization_barrier(halve(keep.reshape(shape), got, Z if split == 'y' else 1))
        got = swap(send, NEXT[split][Z])
        keeps.append(keep)
        gots.append(got)
        fars.append(swap(keep[1] + got[1], NEXT[split][1]))
    return final(keeps, gots, fars, flip)


def final_kernel(flip, *refs):
    count, edge = len(refs) // 3, Z
    for index in range(count):
        keep, got, far = refs[index:-1:count]
        total = (keep[Z] + got[Z] + far[...]) / 16
        cut = slice(edge, edge + total.shape[1])
        edge = cut.stop
        if flip:
            refs[-1][cut, :] = total.T
        else:
            refs[-1][:, cut] = total


def final(keeps, gots, fars, flip):
    shape = (fars[Z].shape[Z], sum(far.shape[1] for far in fars))
    shape = shape[::-1] if flip else shape
    two = [pl.BlockSpec((1, *far.shape), lambda n: (Z, Z, Z)) for far in fars]
    one = [pl.BlockSpec(far.shape, lambda n: (Z, Z)) for far in fars]
    return pl.pallas_call(
        functools.partial(final_kernel, flip), grid=(1,), name='final', in_specs=two + two + one,
        out_specs=pl.BlockSpec(shape, lambda n: (Z, Z)), out_shape=jax.ShapeDtypeStruct(shape, F32),
        cost_estimate=timed(4), compiler_params=ALL_VMEM)(*keeps, *gots, *fars)


def small_kernel(bits_ref, *refs):
    right = refs[2][...]
    for core in range(2):
        refs[3 + core][Z] = tn(refs[core][...], right)


def small_grad(bits, left, right):
    def column(core):
        return lambda k, m: (Z, ((k % 2) ^ m[Z]) * 8 + ((k // 2 % 2) ^ m[1]) * 4 + ((k // 4) ^ m[2]) * 2 + (core ^ m[3]))

    out = pl.BlockSpec((1, LANES, WIDE), lambda k, m: (k, Z, Z))
    grid_spec = pltpu.PrefetchScalarGridSpec(
        num_scalar_prefetch=1, grid=(8,),
        in_specs=[pl.BlockSpec((MODEL, LANES), column(core)) for core in range(2)] + [pl.BlockSpec((MODEL, WIDE), lambda k, m: (Z, Z))],
        out_specs=[out, out])
    keep, send = pl.pallas_call(small_kernel, grid_spec=grid_spec, name='small', out_shape=[jax.ShapeDtypeStruct((8, LANES, WIDE), F32)] * 2,
                                cost_estimate=timed(8), compiler_params=ALL_VMEM)(bits, left, left, right)
    for link in 'cxy':
        got, half = swap(send, link), keep.shape[Z] // 2
        send, keep = lax.optimization_barrier((keep[half:] + got[half:], keep[:half] + got[:half]))
    return (keep[Z] + swap(send, 'z')[Z]) / 16


def join_kernel(*refs):
    row = Z
    for chunk in range(Z, len(refs) - 1, 4):
        rows = slice(row, row + refs[chunk].shape[Z])
        row = rows.stop
        for color in range(2):
            total, far = refs[chunk + 2 * color:chunk + 2 * color + 2]
            refs[-1][rows, :, CHUNK * color:CHUNK * (color + 1)] = (total[...] + far[...]).astype(BF)


def join(parts):
    return pl.pallas_call(join_kernel, name='join', out_shape=jax.ShapeDtypeStruct((16, LANES, WIDE), BF),
                          cost_estimate=timed(4), compiler_params=ALL_VMEM)(*parts)


def gather_kv(kv, order):
    held = {Z: kv}
    for link in order:
        held.update({pos ^ BITS[link]: swap(tile, link) for pos, tile in list(held.items())})
    return [held[pos] for pos in range(8)]


def reduce_dkv(keep, send):
    got = swap(send, 'c')
    parts = []
    for color, (first, second) in enumerate((('x', 'y'), ('y', 'x'))):
        more = swap(keep[color, 1] + got[color, 1], first)
        send, total = lax.optimization_barrier(tuple(keep[color, Z, k] + got[color, Z, k] + more[k] for k in (1, Z)))
        parts += [total, swap(send, second)]
    return parts


CHUNKS = ((Z, 8), (8, 4), (12, 4))
PLAN_UP = (('z', 4), ('y', 4), ('x', 3))
PLAN_D = (('z', 2), ('y', 1), ('x', 1))
PLAN_DOWN = (('z', 3), ('y', 3), ('x', 2))


def solution(mesh):
    def per_device(x_loc, cot_loc, w_q, w_k, w_v, w_o, w_up, w_down):
        batch, seq, d_model = x_loc.shape
        tokens = batch * seq
        me = lax.axis_index('cp').astype(jnp.int32)
        me_one = me.reshape(1)
        bits = jnp.stack([lax.axis_index('dp').astype(jnp.int32), me >> 2, (me >> 1) & 1, me & 1])
        x2, cot2 = x_loc.reshape(tokens, d_model), cot_loc.reshape(tokens, d_model)
        w_q2, w_k2, w_v2, w_o2 = (w.transpose(1, 2, Z).reshape(-1, d_model) for w in (w_q, w_k, w_v, w_o))

        kvs = [kv.reshape(batch // 2, seq, -1) for kv in kv_call(x2, w_k2, w_v2)]
        gathered = [gather_kv(kvs[Z], 'xyc'), gather_kv(kvs[1], 'yxc')]
        q = mm(x2, w_q2, WIDE, Z, 2, SEQ).reshape(batch, seq, -1)
        grad_act = mm(cot2, w_down, WIDE, Z, 4, FF_TILE)

        o, lse_first = attn_fwd(me_one, q, gathered[Z], Z, batch)
        o, lse_second = attn_fwd(me_one, q, gathered[1], batch // 2, batch, o)
        lse = [lse_first, lse_second]
        o2 = o.reshape(tokens, -1)
        h = mm(o2, w_o2, WIDE, Z, 2, SEQ, False, x2)

        act_t, grad_u = ff_block(bits, h, w_up, grad_act)
        grad_w_up = weight_grad(h, grad_u, PLAN_UP, WIDE, Z)
        grad_w_down = weight_grad(act_t.reshape(8, 2, -1, tokens), cot2, PLAN_DOWN, CHUNK, 1)
        grad_h = mm(grad_u, w_up, WIDE, Z, 4, WIDE, True, cot2)
        grad_o = mm(grad_h, w_o2, WIDE, Z, 2, SEQ).reshape(batch, seq, -1)

        grad_q, grad_kv = None, []
        for first, count in CHUNKS:
            side, sub = first // 8, first % 8
            grad_q, keep, send = attn_bwd(me_one, q, grad_o, lse[side], gathered[side], first, sub, count, grad_q)
            grad_kv += reduce_dkv(keep, send)
        grad_q2 = grad_q.reshape(tokens, -1)
        grad_w_o = weight_grad(grad_h, o2, PLAN_D, WIDE, 2, True)
        grad_w_q = weight_grad(x2, grad_q2, PLAN_D, WIDE, 3, True)
        grad_kv2 = join(grad_kv).reshape(tokens, -1)
        grad_w_kv = small_grad(bits, x2, grad_kv2).reshape(-1, 4, 2, HALF)
        grad_x = None
        for part in range(2):
            grad_x = gx_call(grad_h, grad_q2, grad_kv2, w_q2, w_k2, w_v2, part, grad_x)
        return (grad_x.reshape(x_loc.shape), grad_w_q.reshape(32, HALF, -1).transpose(2, Z, 1), grad_w_kv[:, :, Z], grad_w_kv[:, :, 1],
                grad_w_o.reshape(32, HALF, -1).transpose(2, Z, 1), grad_w_up, grad_w_down)

    act_spec = P('dp', 'cp', None)
    rep_three, rep_two = P(None, None, None), P(None, None)
    grad_three, grad_two = P(('dp', 'cp'), None, None), P(('dp', 'cp'), None)
    return jax.shard_map(per_device, mesh=mesh,
                         in_specs=(act_spec, act_spec, rep_three, rep_three, rep_three, rep_three, rep_two, rep_two),
                         out_specs=(act_spec, grad_three, grad_three, grad_three, grad_three, grad_two, grad_two),
                         check_vma=False)
```

```python
import functools, math
import jax, jax.numpy as jnp
from jax import lax
from jax.experimental import pallas as pl
from jax.experimental.pallas import tpu as pltpu
from jax.sharding import PartitionSpec as P


BF, F32 = jnp.bfloat16, jnp.float32
NEG_BIG = -1e30
LANES, WIDE, MODEL, FF_TILE, FF_ROWS, SEQ, Z = 128, 512, 2048, 1408, 352, 1024, 0
HALF = 64
CHUNK = 256
HEADS = 2
NORM = True


def nt(a, b):
    return lax.dot_general(a, b, (((1,), (1,)), ((), ())), preferred_element_type=F32)


def tn(a, b):
    return lax.dot_general(a, b, (((Z,), (Z,)), ((), ())), preferred_element_type=F32)


def nn(a, b):
    return lax.dot_general(a, b, (((1,), (Z,)), ((), ())), preferred_element_type=F32)


def low_lanes(rows):
    return lax.broadcasted_iota(jnp.int32, (rows, LANES), 1) < HALF


def load_keys(me, kv_refs, keys, vals, head):
    low = low_lanes(LANES)
    for pos, ref in enumerate(kv_refs):
        dev = me ^ pos
        tile = ref[Z, :, LANES * head:LANES * (head + 1)]
        flipped = jnp.concatenate([tile[:, HALF:], tile[:, :HALF]], axis=1)
        k_two = jnp.where(low, tile, flipped)
        v_two = jnp.where(low, flipped, tile)
        first = pl.multiple_of(dev * HALF, HALF)
        second = pl.multiple_of((15 - dev) * HALF, HALF)
        keys[pl.ds(first, HALF), :] = k_two[:HALF]
        keys[pl.ds(second, HALF), :] = k_two[HALF:]
        vals[pl.ds(first, HALF), :] = v_two[:HALF]
        vals[pl.ds(second, HALF), :] = v_two[HALF:]


def spread_heads(rows):
    low = low_lanes(HALF)
    zero = jnp.zeros((HALF, LANES), BF)
    parts = []
    for pair in range(4):
        tile = rows[:, LANES * pair:LANES * (pair + 1)]
        parts += [jnp.where(low, tile, zero), jnp.where(low, zero, tile)]
    return jnp.concatenate(parts, axis=Z)


def gather_heads(cols, ref, base, lane):
    low = low_lanes(HALF)
    for pair in range(4):
        tile = cols[:, LANES * pair:LANES * (pair + 1)].T
        ref[Z, base:base + HALF, lane + LANES * pair:lane + LANES * (pair + 1)] = jnp.where(low, tile[:HALF], tile[HALF:]).astype(BF)


def tile_plan(me):
    late = me >= 4
    fifth_key = pl.multiple_of(jnp.where(late, CHUNK, 768), CHUNK)
    fifth_block = jnp.where(late, me, 15 - me)
    return late, [(Z, me, True, Z), (Z, 15 - me, False, 1), (CHUNK, 15 - me, False, 1),
                  (2 * CHUNK, 15 - me, True, 1), (fifth_key, fifth_block, True, 2)]


def lag():
    row = lax.broadcasted_iota(jnp.int32, (CHUNK, WIDE), Z)
    col = lax.broadcasted_iota(jnp.int32, (CHUNK, WIDE), 1)
    return row - (col & (HALF - 1))


def fwd_kernel(scale2, aliased, me_ref, q_ref, *refs):
    kv_refs = refs[:8]
    refs = refs[8 + (1 if aliased else Z):]
    o_ref, lse_ref, keys, vals = refs
    me = me_ref[Z]
    gap = lag()
    late, plan = tile_plan(me)

    def choose(one, two):
        return [one, two, jnp.where(late, one, two)]

    def split(parts):
        zero = jnp.zeros_like(parts[4])
        return parts[Z] + jnp.where(late, parts[4], zero), parts[1] + parts[2] + parts[3] + jnp.where(late, zero, parts[4])

    class Head:
        pass

    heads = []
    for head in range(HEADS):
        x = Head()
        load_keys(me, kv_refs, keys.at[head], vals.at[head], head)
        lanes = slice(WIDE * head, WIDE * (head + 1))
        q_tile = q_ref[Z, :, lanes]
        x.q = choose(spread_heads(q_tile[:HALF]), spread_heads(q_tile[HALF:]))
        x.scores, x.tops, x.exps, x.sums, x.outs = [], [], [], [], []
        heads.append(x)

    def score(head, i):
        x = heads[head]
        start, block, masked, which = plan[i]
        s = nt(keys[head, pl.ds(start, CHUNK), :], x.q[which])
        if masked:
            s = jnp.where(gap <= block * HALF - start, s, NEG_BIG)
        x.scores.append(s)
        x.tops.append(jnp.max(s, axis=Z, keepdims=True))

    def top(head):
        x = heads[head]
        t = x.tops
        top_b = jnp.maximum(jnp.maximum(t[1], t[2]), t[3])
        top_a = jnp.where(late, jnp.maximum(t[Z], t[4]), t[Z]) * scale2
        top_b = jnp.where(late, top_b, jnp.maximum(top_b, t[4])) * scale2
        x.top = choose(top_a, top_b)

    def expo(head, i):
        x = heads[head]
        e = jnp.exp2(x.scores[i] * scale2 - x.top[plan[i][3]])
        x.exps.append(e if NORM else e.astype(BF))
        x.sums.append(jnp.sum(e, axis=Z, keepdims=True))

    def total(head):
        x = heads[head]
        sum_a, sum_b = split(x.sums)
        lse_ref[head, Z:1, :] = x.top[Z] + jnp.log2(sum_a)
        lse_ref[head, 1:2, :] = x.top[1] + jnp.log2(sum_b)
        x.inv = choose(1.0 / sum_a, 1.0 / sum_b)

    def value(head, i):
        x = heads[head]
        p = (x.exps[i] * x.inv[plan[i][3]]).astype(BF) if NORM else x.exps[i]
        x.outs.append(tn(vals[head, pl.ds(plan[i][Z], CHUNK), :], p))

    def finish(head):
        x = heads[head]
        out_a, out_b = split(x.outs)
        if not NORM:
            out_a, out_b = out_a * x.inv[Z], out_b * x.inv[1]
        gather_heads(out_a, o_ref, Z, WIDE * head)
        gather_heads(out_b, o_ref, HALF, WIDE * head)

    n = len(plan)
    for head in range(HEADS + 2):
        for i in range(n):
            if head < HEADS:
                score(head, i)
            if Z <= head - 1 < HEADS:
                if i == Z:
                    top(head - 1)
                expo(head - 1, i)
            if Z <= head - 2 < HEADS:
                if i == Z:
                    total(head - 2)
                value(head - 2, i)
        if Z <= head - 2 < HEADS:
            finish(head - 2)


def bwd_kernel(scale, scale2, aliased, me_ref, q_ref, g_ref, lse_ref, *refs):
    kv_refs = refs[:8]
    refs = refs[8 + (1 if aliased else Z):]
    dq_ref, keep_ref, send_ref, keys, vals, grads = refs
    me = me_ref[Z]
    gap = lag()
    late, plan = tile_plan(me)
    low = low_lanes(CHUNK)

    def choose(one, two):
        return [one, two, jnp.where(late, one, two)]

    def split(parts):
        zero = jnp.zeros_like(parts[4])
        return parts[Z] + jnp.where(late, parts[4], zero), parts[1] + parts[2] + parts[3] + jnp.where(late, zero, parts[4])

    class Head:
        pass

    heads = []
    for head in range(HEADS):
        x = Head()
        load_keys(me, kv_refs, keys.at[head], vals.at[head], head)
        lanes = slice(WIDE * head, WIDE * (head + 1))
        q_tile, g_tile = q_ref[Z, :, lanes], g_ref[Z, :, lanes]
        x.q = choose(spread_heads(q_tile[:HALF]), spread_heads(q_tile[HALF:]))
        x.g = choose(spread_heads(g_tile[:HALF]), spread_heads(g_tile[HALF:]))
        x.lse = choose(lse_ref[head, Z:1, :], lse_ref[head, 1:2, :])
        x.probs, x.dprobs, x.deltas, x.dqs, x.dks, x.dvs = [], [], [], [], [], []
        heads.append(x)

    def prob(head, i):
        x = heads[head]
        start, block, masked, which = plan[i]
        s = nt(keys[head, pl.ds(start, CHUNK), :], x.q[which])
        if masked:
            s = jnp.where(gap <= block * HALF - start, s, NEG_BIG)
        p = jnp.exp2(s * scale2 - x.lse[which])
        dp = nt(vals[head, pl.ds(start, CHUNK), :], x.g[which]).astype(BF)
        x.probs.append(p)
        x.dprobs.append(dp)
        x.deltas.append(jnp.sum(p * dp.astype(F32), axis=Z, keepdims=True))

    def delta(head):
        x = heads[head]
        x.delta = choose(*split(x.deltas))

    def grad(head, i):
        x = heads[head]
        start, _, _, which = plan[i]
        p, dp = x.probs[i], x.dprobs[i]
        ds = (p * (dp.astype(F32) - x.delta[which])).astype(BF)
        x.dvs.append(nn(p.astype(BF), x.g[which]))
        x.dks.append(nn(ds, x.q[which]))
        x.dqs.append(tn(keys[head, pl.ds(start, CHUNK), :], ds))

    def finish(head):
        x = heads[head]
        dq_a, dq_b = split(x.dqs)
        gather_heads(dq_a * scale, dq_ref, Z, WIDE * head)
        gather_heads(dq_b * scale, dq_ref, HALF, WIDE * head)
        zero = jnp.zeros_like(x.dks[4])

        def by_chunk(parts):
            return [parts[Z] + parts[1], parts[2] + jnp.where(late, parts[4], zero), parts[3],
                    jnp.where(late, zero, parts[4])]

        for chunk, (dk, dv) in enumerate(zip(by_chunk(x.dks), by_chunk(x.dvs))):
            dk = (dk + pltpu.roll(dk, HALF, 1)) * scale
            dv = dv + pltpu.roll(dv, HALF, 1)
            both = jnp.where(low, dk, dv)
            for sub in range(4):
                block = 4 * chunk + sub
                dev, base = (block, Z) if block < 8 else (15 - block, HALF)
                grads[dev ^ me, base:base + HALF, LANES * head:LANES * (head + 1)] = both[sub * HALF:(sub + 1) * HALF]

    n = len(plan)
    for head in range(HEADS + 1):
        for i in range(n):
            if head < HEADS:
                prob(head, i)
            if head >= 1:
                if i == Z:
                    delta(head - 1)
                grad(head - 1, i)
        if head >= 1:
            finish(head - 1)
    for one in range(2):
        for two in range(2):
            slot = jnp.where(pl.program_id(1) == Z, 2 * two + one, 2 * one + two)
            keep_ref[Z, one, two, Z] = grads[2 * slot]
            send_ref[Z, one, two, Z] = grads[2 * slot + 1]


def attn_fwd(me, q, kvs, first, total, o_prev=None):
    count = kvs[Z].shape[Z]
    scale2 = 0.125 * math.log2(math.e)
    aliased = o_prev is not None
    row = lambda b, g, m: (first + b, Z, g)
    kv_spec = pl.BlockSpec((1, LANES, LANES * HEADS), lambda b, g, m: (b, Z, g))
    grid_spec = pltpu.PrefetchScalarGridSpec(
        num_scalar_prefetch=1, grid=(count, 4 // HEADS),
        in_specs=[pl.BlockSpec((1, LANES, WIDE * HEADS), row)] + [kv_spec] * 8 + ([pl.BlockSpec(memory_space=pl.ANY)] if aliased else []),
        out_specs=[pl.BlockSpec((1, LANES, WIDE * HEADS), row), pl.BlockSpec((HEADS, 2, WIDE), lambda b, g, m: (b * (4 // HEADS) + g, Z, Z))],
        scratch_shapes=[pltpu.VMEM((HEADS, SEQ, LANES), BF), pltpu.VMEM((HEADS, SEQ, LANES), BF)])
    return pl.pallas_call(
        functools.partial(fwd_kernel, scale2, aliased), grid_spec=grid_spec, name='attn_fwd',
        out_shape=[jax.ShapeDtypeStruct((total, LANES, MODEL), BF), jax.ShapeDtypeStruct((count * 4, 2, WIDE), F32)],
        input_output_aliases={10: Z} if aliased else {},
        cost_estimate=timed(6 * count),
        compiler_params=ALL_VMEM,
    )(me, q, *kvs, *([o_prev] if aliased else []))


def attn_bwd(me, q, g, lse, kvs, first, sub, count, dq_prev=None):
    total = q.shape[Z]
    scale = 0.125
    scale2 = scale * math.log2(math.e)
    aliased = dq_prev is not None
    row = lambda b, h, m: (first + b, Z, h)
    kv_spec = pl.BlockSpec((1, LANES, LANES * HEADS), lambda b, h, m: (sub + b, Z, h))
    part = pl.BlockSpec((1, 2, 2, 1, LANES, CHUNK), lambda b, h, m: (h, Z, Z, b, Z, Z))
    part_shape = jax.ShapeDtypeStruct((2, 2, 2, count, LANES, CHUNK), F32)
    grid_spec = pltpu.PrefetchScalarGridSpec(
        num_scalar_prefetch=1, grid=(count, 4 // HEADS),
        in_specs=[pl.BlockSpec((1, LANES, WIDE * HEADS), row), pl.BlockSpec((1, LANES, WIDE * HEADS), row),
                  pl.BlockSpec((HEADS, 2, WIDE), lambda b, h, m: ((sub + b) * (4 // HEADS) + h, Z, Z))] + [kv_spec] * 8
        + ([pl.BlockSpec(memory_space=pl.ANY)] if aliased else []),
        out_specs=[pl.BlockSpec((1, LANES, WIDE * HEADS), row), part, part],
        scratch_shapes=[pltpu.VMEM((HEADS, SEQ, LANES), BF), pltpu.VMEM((HEADS, SEQ, LANES), BF), pltpu.VMEM((8, LANES, LANES * HEADS), F32)])
    return pl.pallas_call(
        functools.partial(bwd_kernel, scale, scale2, aliased), grid_spec=grid_spec, name='attn_bwd',
        out_shape=[jax.ShapeDtypeStruct((total, LANES, MODEL), BF)] + [part_shape] * 2,
        input_output_aliases={12: Z} if aliased else {},
        cost_estimate=timed(10 * count),
        compiler_params=ALL_VMEM,
    )(me, q, g, lse, *kvs, *([dq_prev] if aliased else []))


BITS = {'c': 1, 'x': 2, 'y': 4}
ALL_VMEM = pltpu.CompilerParams(vmem_limit_bytes=63 * 2**20)
NEXT = {'x': ('y', 'z'), 'y': ('z', 'x'), 'z': ('x', 'y')}


def swap(values, link):
    if link == 'z':
        return lax.ppermute(values, 'dp', [(Z, 1), (1, Z)])
    return lax.ppermute(values, 'cp', [(i, i ^ BITS[link]) for i in range(8)])


def pick(values, axis, index):
    return lax.index_in_dim(values, index, axis, keepdims=False)


def timed(micros):
    return pl.CostEstimate(flops=int(micros * 9e8), bytes_accessed=1 << 20, transcendentals=Z)


def mm_kernel(product, added, x_ref, w_ref, *refs):
    total = product(x_ref[...], w_ref[...])
    if added:
        total = total + refs[Z][...].astype(F32)
    refs[-1][...] = total.astype(refs[-1].dtype)


def mm(x, w, rows, first, count, width, flip=True, added=None, dtype=BF):
    total, depth = x.shape
    tile = pl.BlockSpec((rows, width), lambda n, t: (t, n))
    w_spec = pl.BlockSpec((width, depth), lambda n, t: (first + n, Z)) if flip else pl.BlockSpec(
        (depth, width), lambda n, t: (Z, first + n))
    return pl.pallas_call(
        functools.partial(mm_kernel, nt if flip else nn, added is not None), grid=(count, total // rows), name='mm',
        in_specs=[pl.BlockSpec((rows, depth), lambda n, t: (t, Z)), w_spec] + ([tile] if added is not None else []),
        out_specs=tile, out_shape=jax.ShapeDtypeStruct((total, count * width), dtype),
        cost_estimate=timed(total * count * width * depth * 2 / 9e8),
        compiler_params=ALL_VMEM)(x, w, *([added] if added is not None else []))


def join_kv(k_ref, v_ref, both):
    @pl.when(pl.program_id(Z) == Z)
    def _():
        for head in range(4):
            both[LANES * head:LANES * head + HALF, :] = k_ref[HALF * head:HALF * head + HALF, :]
            both[LANES * head + HALF:LANES * head + LANES, :] = v_ref[HALF * head:HALF * head + HALF, :]


def kv_kernel(x_ref, k_ref, v_ref, low_ref, high_ref, both):
    join_kv(k_ref, v_ref, both)
    value = nt(x_ref[...], both[...]).astype(BF)
    for index, ref in enumerate((low_ref, high_ref)):
        @pl.when(pl.program_id(Z) // 2 == index)
        def _():
            ref[...] = value


def kv_call(x, w_k, w_v):
    rows, (total, depth) = WIDE, x.shape
    whole = pl.BlockSpec((CHUNK, depth), lambda t: (Z, Z), pipeline_mode=pl.Buffered(1))
    return pl.pallas_call(
        kv_kernel, grid=(total // rows,), name='kv',
        in_specs=[pl.BlockSpec((rows, depth), lambda t: (t, Z)), whole, whole],
        out_specs=[pl.BlockSpec((rows, WIDE), lambda t: (jnp.minimum(t, 1), Z)), pl.BlockSpec((rows, WIDE), lambda t: (jnp.maximum(t - 2, Z), Z))],
        out_shape=[jax.ShapeDtypeStruct((total // 2, WIDE), BF)] * 2,
        scratch_shapes=[pltpu.VMEM((WIDE, depth), BF)], cost_estimate=timed(9), compiler_params=ALL_VMEM)(x, w_k, w_v)


def gx_kernel(h_ref, q_ref, g_ref, w_ref, k_ref, v_ref, *refs):
    out_ref, both = refs[-2:]
    join_kv(k_ref, v_ref, both)
    total = nn(q_ref[...], w_ref[...]) + nn(g_ref[...], both[...])
    out_ref[...] = (h_ref[...].astype(F32) + total).astype(BF)


def gx_call(grad_h, grad_q, grad_kv, w_q, w_k, w_v, half, prev=None):
    rows, (total, depth) = WIDE, grad_h.shape
    width = depth // 2
    aliased = prev is not None
    tile = pl.BlockSpec((rows, width), lambda t: (t, half))
    once = lambda count: pl.BlockSpec((count, width), lambda t: (Z, half), pipeline_mode=pl.Buffered(1))
    return pl.pallas_call(
        gx_kernel, grid=(total // rows,), name='gx',
        in_specs=[tile, pl.BlockSpec((rows, depth), lambda t: (t, Z)), pl.BlockSpec((rows, WIDE), lambda t: (t, Z)), once(depth), once(CHUNK),
                  once(CHUNK)] + ([pl.BlockSpec(memory_space=pl.ANY)] if aliased else []),
        out_specs=tile, out_shape=jax.ShapeDtypeStruct((total, depth), BF), scratch_shapes=[pltpu.VMEM((WIDE, width), BF)],
        input_output_aliases={6: Z} if aliased else {}, cost_estimate=timed(14), compiler_params=ALL_VMEM,
    )(grad_h, grad_q, grad_kv, w_q, w_k, w_v, *([prev] if aliased else []))


def ff_kernel(bits_ref, h_ref, w_ref, ga_ref, at_ref, gu_ref, held, turned):
    root = math.sqrt(2.0 / math.pi)
    width = w_ref.shape[1]
    for lo in range(Z, width, CHUNK):
        cut = slice(lo, min(lo + CHUNK, width))
        u = held[:, cut]
        held[:, cut] = nn(h_ref[...], w_ref[:, cut])
        rise = (root * 0.044715) * (u * u)
        t = jnp.tanh(u * (root + rise))
        up, down, half_u = 1.0 + t, 1.0 - t, 0.5 * u
        slope = up * (0.5 + (half_u * down) * (root + 3.0 * rise))
        gu_ref[:, cut] = (ga_ref[:, cut].astype(F32) * slope).astype(BF)
        turned[cut, :] = (half_u * up).T.astype(BF)
    for x in range(2):
        for c in range(2):
            lo = (2 * x + c) * FF_ROWS
            at_ref[Z, Z, x ^ bits_ref[2], c ^ bits_ref[3]] = turned[lo:lo + FF_ROWS, :]


def ff_block(bits, h, w_up, ga):
    tokens, width, rows = MODEL, FF_TILE, WIDE
    per = tokens // rows
    steps = 4 * per
    now = lambda i: jnp.minimum(i, steps - 1)
    then = lambda i: jnp.maximum(i - 1, Z)
    grid_spec = pltpu.PrefetchScalarGridSpec(
        num_scalar_prefetch=1, grid=(steps + 1,),
        in_specs=[pl.BlockSpec((rows, MODEL), lambda i, m: (now(i) % per, Z)),
                  pl.BlockSpec((MODEL, width), lambda i, m: (Z, now(i) // per)),
                  pl.BlockSpec((rows, width), lambda i, m: (then(i) % per, then(i) // per))],
        out_specs=[pl.BlockSpec((1, 1, 2, 2, FF_ROWS, rows), lambda i, m: ((then(i) // per // 2) ^ m[Z], (then(i) // per % 2) ^ m[1], Z, Z, Z, then(i) % per)),
                   pl.BlockSpec((rows, width), lambda i, m: (then(i) % per, then(i) // per))],
        scratch_shapes=[pltpu.VMEM((rows, width), F32), pltpu.VMEM((width, rows), BF)])
    return pl.pallas_call(
        ff_kernel, grid_spec=grid_spec, name='ff_block',
        out_shape=[jax.ShapeDtypeStruct((2, 2, 2, 2, FF_ROWS, tokens), BF), jax.ShapeDtypeStruct((tokens, 5632), BF)],
        cost_estimate=timed(60), compiler_params=ALL_VMEM)(bits, h, w_up, ga)


def color_of(n, plan):
    edge, color = Z, Z
    for _, count in plan[:-1]:
        edge += count
        color = color + (n >= edge).astype(jnp.int32)
    return color


def pair_kernel(plan, rows, turned, *refs):
    n, steps = pl.program_id(Z), sum(count for _, count in plan)
    count = len(plan)
    if turned:
        left, refs = refs[Z], refs[1:]
        take = lambda place, core: left[place, core]
    else:
        parts, left, refs = refs[:16], refs[-1], refs[16:-1]

        @pl.when(n == Z)
        def _():
            for place in range(8):
                for core in range(2):
                    left[place, core] = parts[2 * place + core][...].T

        take = lambda place, core: left[place, core]
    right, outs = refs[Z], refs[1:1 + 2 * count]
    mine, sent, came, send_sem, recv_sem, free_sem = refs[1 + 2 * count:]
    me = lax.axis_index('cp')
    other = {'cp': me + 1 - 2 * (me % 2)}
    mesh_id = pl.DeviceIdType.MESH
    now, then = n % 2, (n + 1) % 2

    def copy(slot):
        return pltpu.make_async_remote_copy(src_ref=sent.at[slot], dst_ref=came.at[slot], send_sem=send_sem.at[slot],
                                            recv_sem=recv_sem.at[slot], device_id=other, device_id_type=mesh_id)

    @pl.when(n == Z)
    def _():
        barrier = pltpu.get_barrier_semaphore()
        pl.semaphore_signal(barrier, inc=1, device_id=other, device_id_type=mesh_id)
        pl.semaphore_wait(barrier, 1)

    @pl.when(n >= 3)
    def _():
        pl.semaphore_wait(free_sem, 1)

    @pl.when(n >= 1)
    def _():
        copy(then).start()

    @pl.when(n < steps)
    def _():
        some = 1 if turned else 4
        for core, dest in ((1, sent), (Z, mine)):
            for place in range(Z, 8, some):
                tile = jnp.concatenate([take(place + k, core) for k in range(some)], axis=Z)
                dest[now, place:place + some] = nn(tile, right[...]).reshape(some, rows, -1)

    @pl.when(n >= 1)
    def _():
        copy(then).wait()
        color = color_of(n - 1, plan)
        for index, (split, _) in enumerate(plan):
            @pl.when(color == index)
            def _():
                for place in range(8):
                    z, y, x = place // 4, place // 2 % 2, place % 2
                    half, k = {'z': (z, 2 * y + x), 'y': (y, 2 * z + x), 'x': (x, 2 * z + y)}[split]
                    outs[2 * index + 1 - half][k] = mine[then, place] + came[then, place]

    @pl.when((n >= 1) & (n < steps - 1))
    def _():
        pl.semaphore_signal(free_sem, inc=1, device_id=other, device_id_type=mesh_id)


def pair_call(left, right, plan, tile, call_id):
    turned = left.ndim == 4
    rows = left.shape[2] if turned else LANES
    steps = sum(count for _, count in plan)
    once = pl.Buffered(1)
    if turned:
        left_specs = [pl.BlockSpec((8, 2, rows, MODEL), lambda n: (Z, Z, Z, Z), pipeline_mode=once)]
    else:
        def column(place, core):
            def at(n):
                me = lax.axis_index('cp')
                bits = (lax.axis_index('dp'), me // 4, (me // 2) % 2, me % 2)
                flips = (place // 4, place // 2 % 2, place % 2, core)
                return Z, sum((1 - bit if flip else bit) * weight for bit, flip, weight in zip(bits, flips, (8, 4, 2, 1)))

            return at

        left_specs = [pl.BlockSpec((MODEL, LANES), column(place, core), pipeline_mode=once) for place in range(8) for core in range(2)]
    out_specs, out_shape, edge = [], [], Z
    for _, count in plan:
        spec = pl.BlockSpec((4, rows, tile), lambda n, edge=edge, count=count: (Z, Z, jnp.clip(n - 1 - edge, Z, count - 1)))
        out_specs += [spec, spec]
        out_shape += [jax.ShapeDtypeStruct((4, rows, count * tile), F32)] * 2
        edge += count
    both = pltpu.VMEM((2, 8, rows, tile), F32)
    two = pltpu.SemaphoreType.DMA((2,))
    return pl.pallas_call(
        functools.partial(pair_kernel, plan, rows, turned), grid=(steps + 1,), name='pair',
        in_specs=left_specs + [pl.BlockSpec((MODEL, tile), lambda n: (Z, jnp.minimum(n, steps - 1)))], out_specs=out_specs, out_shape=out_shape,
        scratch_shapes=[both, both, both, two, two, pltpu.SemaphoreType.REGULAR] + ([] if turned else [pltpu.VMEM((8, 2, LANES, MODEL), BF)]),
        cost_estimate=timed(16 * rows * steps * tile * 4096 / 9e8),
        compiler_params=pltpu.CompilerParams(vmem_limit_bytes=63 * 2**20, collective_id=call_id, has_side_effects=True),
    )(*([left] * len(left_specs)), right)


def halve(keep, got, axis):
    return tuple(pick(keep, axis, k) + pick(got, axis, k) for k in (1, Z))


def weight_grad(left, right, plan, tile, call_id, flip=False):
    outs = pair_call(left, right, plan, tile, call_id)
    keeps, gots, fars = [], [], []
    for (split, _), send, keep in zip(plan, outs[::2], outs[1::2]):
        shape = (2, 2, *keep.shape[1:])
        got = swap(send, split).reshape(shape)
        send, keep = lax.optimization_barrier(halve(keep.reshape(shape), got, Z if split == 'y' else 1))
        got = swap(send, NEXT[split][Z])
        keeps.append(keep)
        gots.append(got)
        fars.append(swap(keep[1] + got[1], NEXT[split][1]))
    return final(keeps, gots, fars, flip)


def final_kernel(flip, *refs):
    count, edge = len(refs) // 3, Z
    for index in range(count):
        keep, got, far = refs[index:-1:count]
        total = (keep[Z] + got[Z] + far[...]) / 16
        cut = slice(edge, edge + total.shape[1])
        edge = cut.stop
        if flip:
            refs[-1][cut, :] = total.T
        else:
            refs[-1][:, cut] = total


def final(keeps, gots, fars, flip):
    shape = (fars[Z].shape[Z], sum(far.shape[1] for far in fars))
    shape = shape[::-1] if flip else shape
    two = [pl.BlockSpec((1, *far.shape), lambda n: (Z, Z, Z)) for far in fars]
    one = [pl.BlockSpec(far.shape, lambda n: (Z, Z)) for far in fars]
    return pl.pallas_call(
        functools.partial(final_kernel, flip), grid=(1,), name='final', in_specs=two + two + one,
        out_specs=pl.BlockSpec(shape, lambda n: (Z, Z)), out_shape=jax.ShapeDtypeStruct(shape, F32),
        cost_estimate=timed(4), compiler_params=ALL_VMEM)(*keeps, *gots, *fars)


def small_kernel(bits_ref, *refs):
    right = refs[2][...]
    for core in range(2):
        refs[3 + core][Z] = tn(refs[core][...], right)


def small_grad(bits, left, right):
    def column(core):
        return lambda k, m: (Z, ((k % 2) ^ m[Z]) * 8 + ((k // 2 % 2) ^ m[1]) * 4 + ((k // 4) ^ m[2]) * 2 + (core ^ m[3]))

    out = pl.BlockSpec((1, LANES, WIDE), lambda k, m: (k, Z, Z))
    grid_spec = pltpu.PrefetchScalarGridSpec(
        num_scalar_prefetch=1, grid=(8,),
        in_specs=[pl.BlockSpec((MODEL, LANES), column(core)) for core in range(2)] + [pl.BlockSpec((MODEL, WIDE), lambda k, m: (Z, Z))],
        out_specs=[out, out])
    keep, send = pl.pallas_call(small_kernel, grid_spec=grid_spec, name='small', out_shape=[jax.ShapeDtypeStruct((8, LANES, WIDE), F32)] * 2,
                                cost_estimate=timed(8), compiler_params=ALL_VMEM)(bits, left, left, right)
    for link in 'cxy':
        got, half = swap(send, link), keep.shape[Z] // 2
        send, keep = lax.optimization_barrier((keep[half:] + got[half:], keep[:half] + got[:half]))
    return (keep[Z] + swap(send, 'z')[Z]) / 16


def join_kernel(*refs):
    row = Z
    for chunk in range(Z, len(refs) - 1, 4):
        rows = slice(row, row + refs[chunk].shape[Z])
        row = rows.stop
        for color in range(2):
            total, far = refs[chunk + 2 * color:chunk + 2 * color + 2]
            refs[-1][rows, :, CHUNK * color:CHUNK * (color + 1)] = (total[...] + far[...]).astype(BF)


def join(parts):
    return pl.pallas_call(join_kernel, name='join', out_shape=jax.ShapeDtypeStruct((16, LANES, WIDE), BF),
                          cost_estimate=timed(4), compiler_params=ALL_VMEM)(*parts)


def gather_kv(kv, order):
    held = {Z: kv}
    for link in order:
        held.update({pos ^ BITS[link]: swap(tile, link) for pos, tile in list(held.items())})
    return [held[pos] for pos in range(8)]


def reduce_dkv(keep, send):
    got = swap(send, 'c')
    parts = []
    for color, (first, second) in enumerate((('x', 'y'), ('y', 'x'))):
        more = swap(keep[color, 1] + got[color, 1], first)
        send, total = lax.optimization_barrier(tuple(keep[color, Z, k] + got[color, Z, k] + more[k] for k in (1, Z)))
        parts += [total, swap(send, second)]
    return parts


CHUNKS = ((Z, 8), (8, 4), (12, 4))
PLAN_UP = (('z', 4), ('y', 4), ('x', 3))
PLAN_D = (('z', 3), ('y', 3), ('x', 2))


def solution(mesh):
    def per_device(x_loc, cot_loc, w_q, w_k, w_v, w_o, w_up, w_down):
        batch, seq, d_model = x_loc.shape
        tokens = batch * seq
        me = lax.axis_index('cp').astype(jnp.int32)
        me_one = me.reshape(1)
        bits = jnp.stack([lax.axis_index('dp').astype(jnp.int32), me >> 2, (me >> 1) & 1, me & 1])
        x2, cot2 = x_loc.reshape(tokens, d_model), cot_loc.reshape(tokens, d_model)
        w_q2, w_k2, w_v2, w_o2 = (w.transpose(1, 2, Z).reshape(-1, d_model) for w in (w_q, w_k, w_v, w_o))

        kvs = [kv.reshape(batch // 2, seq, -1) for kv in kv_call(x2, w_k2, w_v2)]
        gathered = [gather_kv(kvs[Z], 'xyc'), gather_kv(kvs[1], 'yxc')]
        q = mm(x2, w_q2, WIDE, Z, 2, SEQ).reshape(batch, seq, -1)
        grad_act = mm(cot2, w_down, WIDE, Z, 4, FF_TILE)

        o, lse_first = attn_fwd(me_one, q, gathered[Z], Z, batch)
        o, lse_second = attn_fwd(me_one, q, gathered[1], batch // 2, batch, o)
        lse = [lse_first, lse_second]
        o2 = o.reshape(tokens, -1)
        h = mm(o2, w_o2, WIDE, Z, 2, SEQ, False, x2)

        act_t, grad_u = ff_block(bits, h, w_up, grad_act)
        grad_w_up = weight_grad(h, grad_u, PLAN_UP, WIDE, Z)
        grad_w_down = weight_grad(act_t.reshape(8, 2, -1, tokens), cot2, PLAN_D, CHUNK, 1)
        grad_h = mm(grad_u, w_up, WIDE, Z, 4, WIDE, True, cot2)
        grad_o = mm(grad_h, w_o2, WIDE, Z, 2, SEQ).reshape(batch, seq, -1)

        grad_q, grad_kv = None, []
        for part, (first, count) in enumerate(CHUNKS):
            side, sub = first // 8, first % 8
            grad_q, keep, send = attn_bwd(me_one, q, grad_o, lse[side], gathered[side], first, sub, count, grad_q)
            grad_kv += reduce_dkv(keep, send)
            if part == Z:
                grad_w_o = weight_grad(grad_h, o2, PLAN_D, CHUNK, 2, True)
        grad_q2 = grad_q.reshape(tokens, -1)
        grad_w_q = weight_grad(x2, grad_q2, PLAN_D, CHUNK, 3, True)
        grad_kv2 = join(grad_kv).reshape(tokens, -1)
        grad_w_kv = small_grad(bits, x2, grad_kv2).reshape(-1, 4, 2, HALF)
        grad_x = None
        for part in range(2):
            grad_x = gx_call(grad_h, grad_q2, grad_kv2, w_q2, w_k2, w_v2, part, grad_x)
        return (grad_x.reshape(x_loc.shape), grad_w_q.reshape(32, HALF, -1).transpose(2, Z, 1), grad_w_kv[:, :, Z], grad_w_kv[:, :, 1],
                grad_w_o.reshape(32, HALF, -1).transpose(2, Z, 1), grad_w_up, grad_w_down)

    act_spec = P('dp', 'cp', None)
    rep_three, rep_two = P(None, None, None), P(None, None)
    grad_three, grad_two = P(('dp', 'cp'), None, None), P(('dp', 'cp'), None)
    return jax.shard_map(per_device, mesh=mesh,
                         in_specs=(act_spec, act_spec, rep_three, rep_three, rep_three, rep_three, rep_two, rep_two),
                         out_specs=(act_spec, grad_three, grad_three, grad_three, grad_three, grad_two, grad_two),
                         check_vma=False)
```

```python
import functools, math
import jax, jax.numpy as jnp
from jax import lax
from jax.experimental import pallas as pl
from jax.experimental.pallas import tpu as pltpu
from jax.sharding import PartitionSpec as P


BF, F32 = jnp.bfloat16, jnp.float32
NEG_BIG = -1e30
LANES, WIDE, MODEL, FF_TILE, FF_ROWS, SEQ, Z = 128, 512, 2048, 1408, 352, 1024, 0
HALF = 64
CHUNK = 256
HEADS = 2
NORM = True


def nt(a, b):
    return lax.dot_general(a, b, (((1,), (1,)), ((), ())), preferred_element_type=F32)


def tn(a, b):
    return lax.dot_general(a, b, (((Z,), (Z,)), ((), ())), preferred_element_type=F32)


def nn(a, b):
    return lax.dot_general(a, b, (((1,), (Z,)), ((), ())), preferred_element_type=F32)


def low_lanes(rows):
    return lax.broadcasted_iota(jnp.int32, (rows, LANES), 1) < HALF


def load_keys(me, kv_refs, keys, vals, head):
    low = low_lanes(LANES)
    for pos, ref in enumerate(kv_refs):
        dev = me ^ pos
        tile = ref[Z, :, LANES * head:LANES * (head + 1)]
        flipped = jnp.concatenate([tile[:, HALF:], tile[:, :HALF]], axis=1)
        k_two = jnp.where(low, tile, flipped)
        v_two = jnp.where(low, flipped, tile)
        first = pl.multiple_of(dev * HALF, HALF)
        second = pl.multiple_of((15 - dev) * HALF, HALF)
        keys[pl.ds(first, HALF), :] = k_two[:HALF]
        keys[pl.ds(second, HALF), :] = k_two[HALF:]
        vals[pl.ds(first, HALF), :] = v_two[:HALF]
        vals[pl.ds(second, HALF), :] = v_two[HALF:]


def spread_heads(rows):
    low = low_lanes(HALF)
    zero = jnp.zeros((HALF, LANES), BF)
    parts = []
    for pair in range(4):
        tile = rows[:, LANES * pair:LANES * (pair + 1)]
        parts += [jnp.where(low, tile, zero), jnp.where(low, zero, tile)]
    return jnp.concatenate(parts, axis=Z)


def gather_heads(cols, ref, base, lane):
    low = low_lanes(HALF)
    for pair in range(4):
        tile = cols[:, LANES * pair:LANES * (pair + 1)].T
        ref[Z, base:base + HALF, lane + LANES * pair:lane + LANES * (pair + 1)] = jnp.where(low, tile[:HALF], tile[HALF:]).astype(BF)


def tile_plan(me):
    late = me >= 4
    fifth_key = pl.multiple_of(jnp.where(late, CHUNK, 768), CHUNK)
    fifth_block = jnp.where(late, me, 15 - me)
    return late, [(Z, me, True, Z), (Z, 15 - me, False, 1), (CHUNK, 15 - me, False, 1),
                  (2 * CHUNK, 15 - me, True, 1), (fifth_key, fifth_block, True, 2)]


def lag():
    row = lax.broadcasted_iota(jnp.int32, (CHUNK, WIDE), Z)
    col = lax.broadcasted_iota(jnp.int32, (CHUNK, WIDE), 1)
    return row - (col & (HALF - 1))


def fwd_kernel(scale2, aliased, me_ref, q_ref, *refs):
    kv_refs = refs[:8]
    refs = refs[8 + (1 if aliased else Z):]
    o_ref, lse_ref, keys, vals = refs
    me = me_ref[Z]
    gap = lag()
    late, plan = tile_plan(me)

    def choose(one, two):
        return [one, two, jnp.where(late, one, two)]

    def split(parts):
        zero = jnp.zeros_like(parts[4])
        return parts[Z] + jnp.where(late, parts[4], zero), parts[1] + parts[2] + parts[3] + jnp.where(late, zero, parts[4])

    class Head:
        pass

    heads = []
    for head in range(HEADS):
        x = Head()
        load_keys(me, kv_refs, keys.at[head], vals.at[head], head)
        lanes = slice(WIDE * head, WIDE * (head + 1))
        q_tile = q_ref[Z, :, lanes]
        x.q = choose(spread_heads(q_tile[:HALF]), spread_heads(q_tile[HALF:]))
        x.scores, x.tops, x.exps, x.sums, x.outs = [], [], [], [], []
        heads.append(x)

    def score(head, i):
        x = heads[head]
        start, block, masked, which = plan[i]
        s = nt(keys[head, pl.ds(start, CHUNK), :], x.q[which])
        if masked:
            s = jnp.where(gap <= block * HALF - start, s, NEG_BIG)
        x.scores.append(s)
        x.tops.append(jnp.max(s, axis=Z, keepdims=True))

    def top(head):
        x = heads[head]
        t = x.tops
        top_b = jnp.maximum(jnp.maximum(t[1], t[2]), t[3])
        top_a = jnp.where(late, jnp.maximum(t[Z], t[4]), t[Z]) * scale2
        top_b = jnp.where(late, top_b, jnp.maximum(top_b, t[4])) * scale2
        x.top = choose(top_a, top_b)

    def expo(head, i):
        x = heads[head]
        e = jnp.exp2(x.scores[i] * scale2 - x.top[plan[i][3]])
        x.exps.append(e if NORM else e.astype(BF))
        x.sums.append(jnp.sum(e, axis=Z, keepdims=True))

    def total(head):
        x = heads[head]
        sum_a, sum_b = split(x.sums)
        lse_ref[head, Z:1, :] = x.top[Z] + jnp.log2(sum_a)
        lse_ref[head, 1:2, :] = x.top[1] + jnp.log2(sum_b)
        x.inv = choose(1.0 / sum_a, 1.0 / sum_b)

    def value(head, i):
        x = heads[head]
        p = (x.exps[i] * x.inv[plan[i][3]]).astype(BF) if NORM else x.exps[i]
        x.outs.append(tn(vals[head, pl.ds(plan[i][Z], CHUNK), :], p))

    def finish(head):
        x = heads[head]
        out_a, out_b = split(x.outs)
        if not NORM:
            out_a, out_b = out_a * x.inv[Z], out_b * x.inv[1]
        gather_heads(out_a, o_ref, Z, WIDE * head)
        gather_heads(out_b, o_ref, HALF, WIDE * head)

    n = len(plan)
    for head in range(HEADS + 2):
        for i in range(n):
            if head < HEADS:
                score(head, i)
            if Z <= head - 1 < HEADS:
                if i == Z:
                    top(head - 1)
                expo(head - 1, i)
            if Z <= head - 2 < HEADS:
                if i == Z:
                    total(head - 2)
                value(head - 2, i)
        if Z <= head - 2 < HEADS:
            finish(head - 2)


def bwd_kernel(scale, scale2, aliased, me_ref, q_ref, g_ref, lse_ref, *refs):
    kv_refs = refs[:8]
    refs = refs[8 + (1 if aliased else Z):]
    dq_ref, keep_ref, send_ref, keys, vals, grads = refs
    me = me_ref[Z]
    gap = lag()
    late, plan = tile_plan(me)
    low = low_lanes(CHUNK)

    def choose(one, two):
        return [one, two, jnp.where(late, one, two)]

    def split(parts):
        zero = jnp.zeros_like(parts[4])
        return parts[Z] + jnp.where(late, parts[4], zero), parts[1] + parts[2] + parts[3] + jnp.where(late, zero, parts[4])

    class Head:
        pass

    heads = []
    for head in range(HEADS):
        x = Head()
        load_keys(me, kv_refs, keys.at[head], vals.at[head], head)
        lanes = slice(WIDE * head, WIDE * (head + 1))
        q_tile, g_tile = q_ref[Z, :, lanes], g_ref[Z, :, lanes]
        x.q = choose(spread_heads(q_tile[:HALF]), spread_heads(q_tile[HALF:]))
        x.g = choose(spread_heads(g_tile[:HALF]), spread_heads(g_tile[HALF:]))
        x.lse = choose(lse_ref[head, Z:1, :], lse_ref[head, 1:2, :])
        x.probs, x.dprobs, x.deltas, x.dqs, x.dks, x.dvs = [], [], [], [], [], []
        heads.append(x)

    def prob(head, i):
        x = heads[head]
        start, block, masked, which = plan[i]
        s = nt(keys[head, pl.ds(start, CHUNK), :], x.q[which])
        if masked:
            s = jnp.where(gap <= block * HALF - start, s, NEG_BIG)
        p = jnp.exp2(s * scale2 - x.lse[which])
        dp = nt(vals[head, pl.ds(start, CHUNK), :], x.g[which]).astype(BF)
        x.probs.append(p)
        x.dprobs.append(dp)
        x.deltas.append(jnp.sum(p * dp.astype(F32), axis=Z, keepdims=True))

    def delta(head):
        x = heads[head]
        x.delta = choose(*split(x.deltas))

    def grad(head, i):
        x = heads[head]
        start, _, _, which = plan[i]
        p, dp = x.probs[i], x.dprobs[i]
        ds = (p * (dp.astype(F32) - x.delta[which])).astype(BF)
        x.dvs.append(nn(p.astype(BF), x.g[which]))
        x.dks.append(nn(ds, x.q[which]))
        x.dqs.append(tn(keys[head, pl.ds(start, CHUNK), :], ds))

    def finish(head):
        x = heads[head]
        dq_a, dq_b = split(x.dqs)
        gather_heads(dq_a * scale, dq_ref, Z, WIDE * head)
        gather_heads(dq_b * scale, dq_ref, HALF, WIDE * head)
        zero = jnp.zeros_like(x.dks[4])

        def by_chunk(parts):
            return [parts[Z] + parts[1], parts[2] + jnp.where(late, parts[4], zero), parts[3],
                    jnp.where(late, zero, parts[4])]

        for chunk, (dk, dv) in enumerate(zip(by_chunk(x.dks), by_chunk(x.dvs))):
            dk = (dk + pltpu.roll(dk, HALF, 1)) * scale
            dv = dv + pltpu.roll(dv, HALF, 1)
            both = jnp.where(low, dk, dv)
            for sub in range(4):
                block = 4 * chunk + sub
                dev, base = (block, Z) if block < 8 else (15 - block, HALF)
                grads[dev ^ me, base:base + HALF, LANES * head:LANES * (head + 1)] = both[sub * HALF:(sub + 1) * HALF]

    n = len(plan)
    for head in range(HEADS + 1):
        for i in range(n):
            if head < HEADS:
                prob(head, i)
            if head >= 1:
                if i == Z:
                    delta(head - 1)
                grad(head - 1, i)
        if head >= 1:
            finish(head - 1)
    for one in range(2):
        for two in range(2):
            slot = jnp.where(pl.program_id(1) == Z, 2 * two + one, 2 * one + two)
            keep_ref[Z, one, two, Z] = grads[2 * slot]
            send_ref[Z, one, two, Z] = grads[2 * slot + 1]


def attn_fwd(me, q, kvs, first, total, o_prev=None):
    count = kvs[Z].shape[Z]
    scale2 = 0.125 * math.log2(math.e)
    aliased = o_prev is not None
    row = lambda b, g, m: (first + b, Z, g)
    kv_spec = pl.BlockSpec((1, LANES, LANES * HEADS), lambda b, g, m: (b, Z, g))
    grid_spec = pltpu.PrefetchScalarGridSpec(
        num_scalar_prefetch=1, grid=(count, 4 // HEADS),
        in_specs=[pl.BlockSpec((1, LANES, WIDE * HEADS), row)] + [kv_spec] * 8 + ([pl.BlockSpec(memory_space=pl.ANY)] if aliased else []),
        out_specs=[pl.BlockSpec((1, LANES, WIDE * HEADS), row), pl.BlockSpec((HEADS, 2, WIDE), lambda b, g, m: (b * (4 // HEADS) + g, Z, Z))],
        scratch_shapes=[pltpu.VMEM((HEADS, SEQ, LANES), BF), pltpu.VMEM((HEADS, SEQ, LANES), BF)])
    return pl.pallas_call(
        functools.partial(fwd_kernel, scale2, aliased), grid_spec=grid_spec, name='attn_fwd',
        out_shape=[jax.ShapeDtypeStruct((total, LANES, MODEL), BF), jax.ShapeDtypeStruct((count * 4, 2, WIDE), F32)],
        input_output_aliases={10: Z} if aliased else {},
        cost_estimate=timed(6 * count),
        compiler_params=ALL_VMEM,
    )(me, q, *kvs, *([o_prev] if aliased else []))


def attn_bwd(me, q, g, lse, kvs, first, sub, count, dq_prev=None):
    total = q.shape[Z]
    scale = 0.125
    scale2 = scale * math.log2(math.e)
    aliased = dq_prev is not None
    row = lambda b, h, m: (first + b, Z, h)
    kv_spec = pl.BlockSpec((1, LANES, LANES * HEADS), lambda b, h, m: (sub + b, Z, h))
    part = pl.BlockSpec((1, 2, 2, 1, LANES, CHUNK), lambda b, h, m: (h, Z, Z, b, Z, Z))
    part_shape = jax.ShapeDtypeStruct((2, 2, 2, count, LANES, CHUNK), F32)
    grid_spec = pltpu.PrefetchScalarGridSpec(
        num_scalar_prefetch=1, grid=(count, 4 // HEADS),
        in_specs=[pl.BlockSpec((1, LANES, WIDE * HEADS), row), pl.BlockSpec((1, LANES, WIDE * HEADS), row),
                  pl.BlockSpec((HEADS, 2, WIDE), lambda b, h, m: ((sub + b) * (4 // HEADS) + h, Z, Z))] + [kv_spec] * 8
        + ([pl.BlockSpec(memory_space=pl.ANY)] if aliased else []),
        out_specs=[pl.BlockSpec((1, LANES, WIDE * HEADS), row), part, part],
        scratch_shapes=[pltpu.VMEM((HEADS, SEQ, LANES), BF), pltpu.VMEM((HEADS, SEQ, LANES), BF), pltpu.VMEM((8, LANES, LANES * HEADS), F32)])
    return pl.pallas_call(
        functools.partial(bwd_kernel, scale, scale2, aliased), grid_spec=grid_spec, name='attn_bwd',
        out_shape=[jax.ShapeDtypeStruct((total, LANES, MODEL), BF)] + [part_shape] * 2,
        input_output_aliases={12: Z} if aliased else {},
        cost_estimate=timed(10 * count),
        compiler_params=ALL_VMEM,
    )(me, q, g, lse, *kvs, *([dq_prev] if aliased else []))


BITS = {'c': 1, 'x': 2, 'y': 4}
ALL_VMEM = pltpu.CompilerParams(vmem_limit_bytes=63 * 2**20)
FF_PARAMS = pltpu.CompilerParams(vmem_limit_bytes=63 * 2**20)
NEXT = {'x': ('y', 'z'), 'y': ('z', 'x'), 'z': ('x', 'y')}


def swap(values, link):
    if link == 'z':
        return lax.ppermute(values, 'dp', [(Z, 1), (1, Z)])
    return lax.ppermute(values, 'cp', [(i, i ^ BITS[link]) for i in range(8)])


def pick(values, axis, index):
    return lax.index_in_dim(values, index, axis, keepdims=False)


def timed(micros):
    return pl.CostEstimate(flops=int(micros * 9e8), bytes_accessed=1 << 20, transcendentals=Z)


def mm_kernel(product, added, x_ref, w_ref, *refs):
    total = product(x_ref[...], w_ref[...])
    if added:
        total = total + refs[Z][...].astype(F32)
    refs[-1][...] = total.astype(refs[-1].dtype)


def mm(x, w, rows, first, count, width, flip=True, added=None, dtype=BF):
    total, depth = x.shape
    tile = pl.BlockSpec((rows, width), lambda n, t: (t, n))
    w_spec = pl.BlockSpec((width, depth), lambda n, t: (first + n, Z)) if flip else pl.BlockSpec(
        (depth, width), lambda n, t: (Z, first + n))
    return pl.pallas_call(
        functools.partial(mm_kernel, nt if flip else nn, added is not None), grid=(count, total // rows), name='mm',
        in_specs=[pl.BlockSpec((rows, depth), lambda n, t: (t, Z)), w_spec] + ([tile] if added is not None else []),
        out_specs=tile, out_shape=jax.ShapeDtypeStruct((total, count * width), dtype),
        cost_estimate=timed(total * count * width * depth * 2 / 9e8),
        compiler_params=ALL_VMEM)(x, w, *([added] if added is not None else []))


def join_kv(k_ref, v_ref, both):
    @pl.when(pl.program_id(Z) == Z)
    def _():
        for head in range(4):
            both[LANES * head:LANES * head + HALF, :] = k_ref[HALF * head:HALF * head + HALF, :]
            both[LANES * head + HALF:LANES * head + LANES, :] = v_ref[HALF * head:HALF * head + HALF, :]


def kv_kernel(x_ref, k_ref, v_ref, low_ref, high_ref, both):
    join_kv(k_ref, v_ref, both)
    value = nt(x_ref[...], both[...]).astype(BF)
    for index, ref in enumerate((low_ref, high_ref)):
        @pl.when(pl.program_id(Z) // 2 == index)
        def _():
            ref[...] = value


def kv_call(x, w_k, w_v):
    rows, (total, depth) = WIDE, x.shape
    whole = pl.BlockSpec((CHUNK, depth), lambda t: (Z, Z), pipeline_mode=pl.Buffered(1))
    return pl.pallas_call(
        kv_kernel, grid=(total // rows,), name='kv',
        in_specs=[pl.BlockSpec((rows, depth), lambda t: (t, Z)), whole, whole],
        out_specs=[pl.BlockSpec((rows, WIDE), lambda t: (jnp.minimum(t, 1), Z)), pl.BlockSpec((rows, WIDE), lambda t: (jnp.maximum(t - 2, Z), Z))],
        out_shape=[jax.ShapeDtypeStruct((total // 2, WIDE), BF)] * 2,
        scratch_shapes=[pltpu.VMEM((WIDE, depth), BF)], cost_estimate=timed(9), compiler_params=ALL_VMEM)(x, w_k, w_v)


def gx_kernel(h_ref, q_ref, g_ref, w_ref, k_ref, v_ref, *refs):
    out_ref, both = refs[-2:]
    join_kv(k_ref, v_ref, both)
    total = nn(q_ref[...], w_ref[...]) + nn(g_ref[...], both[...])
    out_ref[...] = (h_ref[...].astype(F32) + total).astype(BF)


def gx_call(grad_h, grad_q, grad_kv, w_q, w_k, w_v, half, prev=None):
    rows, (total, depth) = WIDE, grad_h.shape
    width = depth // 2
    aliased = prev is not None
    tile = pl.BlockSpec((rows, width), lambda t: (t, half))
    once = lambda count: pl.BlockSpec((count, width), lambda t: (Z, half), pipeline_mode=pl.Buffered(1))
    return pl.pallas_call(
        gx_kernel, grid=(total // rows,), name='gx',
        in_specs=[tile, pl.BlockSpec((rows, depth), lambda t: (t, Z)), pl.BlockSpec((rows, WIDE), lambda t: (t, Z)), once(depth), once(CHUNK),
                  once(CHUNK)] + ([pl.BlockSpec(memory_space=pl.ANY)] if aliased else []),
        out_specs=tile, out_shape=jax.ShapeDtypeStruct((total, depth), BF), scratch_shapes=[pltpu.VMEM((WIDE, width), BF)],
        input_output_aliases={6: Z} if aliased else {}, cost_estimate=timed(14), compiler_params=ALL_VMEM,
    )(grad_h, grad_q, grad_kv, w_q, w_k, w_v, *([prev] if aliased else []))


def ff_kernel(bits_ref, h_ref, w_ref, ga_ref, at_ref, gu_ref, held, turned):
    root = math.sqrt(2.0 / math.pi)
    width = w_ref.shape[1]
    for lo in range(Z, width, CHUNK):
        cut = slice(lo, min(lo + CHUNK, width))
        u = held[:, cut]
        held[:, cut] = nn(h_ref[...], w_ref[:, cut])
        rise = (root * 0.044715) * (u * u)
        t = jnp.tanh(u * (root + rise))
        up, down, half_u = 1.0 + t, 1.0 - t, 0.5 * u
        slope = up * (0.5 + (half_u * down) * (root + 3.0 * rise))
        gu_ref[:, cut] = (ga_ref[:, cut].astype(F32) * slope).astype(BF)
        turned[cut, :] = (half_u * up).T.astype(BF)
    for x in range(2):
        for c in range(2):
            lo = (2 * x + c) * FF_ROWS
            at_ref[Z, Z, x ^ bits_ref[2], c ^ bits_ref[3]] = turned[lo:lo + FF_ROWS, :]


def ff_block(bits, h, w_up, ga):
    tokens, width, rows = MODEL, FF_TILE, WIDE
    per = tokens // rows
    steps = 4 * per
    now = lambda i: jnp.minimum(i, steps - 1)
    then = lambda i: jnp.maximum(i - 1, Z)
    grid_spec = pltpu.PrefetchScalarGridSpec(
        num_scalar_prefetch=1, grid=(steps + 1,),
        in_specs=[pl.BlockSpec((rows, MODEL), lambda i, m: (now(i) % per, Z)),
                  pl.BlockSpec((MODEL, width), lambda i, m: (Z, now(i) // per)),
                  pl.BlockSpec((rows, width), lambda i, m: (then(i) % per, then(i) // per))],
        out_specs=[pl.BlockSpec((1, 1, 2, 2, FF_ROWS, rows), lambda i, m: ((then(i) // per // 2) ^ m[Z], (then(i) // per % 2) ^ m[1], Z, Z, Z, then(i) % per)),
                   pl.BlockSpec((rows, width), lambda i, m: (then(i) % per, then(i) // per))],
        scratch_shapes=[pltpu.VMEM((rows, width), F32), pltpu.VMEM((width, rows), BF)])
    return pl.pallas_call(
        ff_kernel, grid_spec=grid_spec, name='ff_block',
        out_shape=[jax.ShapeDtypeStruct((2, 2, 2, 2, FF_ROWS, tokens), BF), jax.ShapeDtypeStruct((tokens, 5632), BF)],
        cost_estimate=timed(60), compiler_params=FF_PARAMS)(bits, h, w_up, ga)


def color_of(n, plan):
    edge, color = Z, Z
    for _, count in plan[:-1]:
        edge += count
        color = color + (n >= edge).astype(jnp.int32)
    return color


def pair_kernel(plan, rows, turned, *refs):
    n, steps = pl.program_id(Z), sum(count for _, count in plan)
    count = len(plan)
    source, left, load_sem = refs[Z], refs[-2], refs[-1]
    parts, refs = (None, refs[1:-2]) if turned else (refs[-3], refs[1:-3])
    me = lax.axis_index('cp')
    bits = (lax.axis_index('dp'), me // 4, (me // 2) % 2, me % 2)

    def load(place, core):
        if turned:
            from_ref, to_ref = source.at[place, core], left.at[place, core]
        else:
            flips = (place // 4, place // 2 % 2, place % 2, core)
            block = sum((1 - bit if flip else bit) * weight for bit, flip, weight in zip(bits, flips, (8, 4, 2, 1)))
            from_ref, to_ref = source.at[:, pl.ds(pl.multiple_of(block * LANES, LANES), LANES)], parts.at[place, core]
        return pltpu.make_async_copy(from_ref, to_ref, load_sem.at[place, core])

    right, outs = refs[Z], refs[1:1 + 2 * count]
    mine, sent, came, send_sem, recv_sem, free_sem = refs[1 + 2 * count:]
    other = {'cp': me + 1 - 2 * (me % 2)}
    mesh_id = pl.DeviceIdType.MESH
    now, then = n % 2, (n + 1) % 2

    def copy(slot):
        return pltpu.make_async_remote_copy(src_ref=sent.at[slot], dst_ref=came.at[slot], send_sem=send_sem.at[slot],
                                            recv_sem=recv_sem.at[slot], device_id=other, device_id_type=mesh_id)

    @pl.when(n == Z)
    def _():
        for core in (1, Z):
            for place in range(8):
                load(place, core).start()
        barrier = pltpu.get_barrier_semaphore()
        pl.semaphore_signal(barrier, inc=1, device_id=other, device_id_type=mesh_id)
        pl.semaphore_wait(barrier, 1)

    @pl.when(n >= 3)
    def _():
        pl.semaphore_wait(free_sem, 1)

    @pl.when(n >= 1)
    def _():
        copy(then).start()

    def products(first):
        some = 1 if turned else 4
        for core, dest in ((1, sent), (Z, mine)):
            for place in range(Z, 8, some):
                group = range(place, place + some)
                if first:
                    for k in group:
                        load(k, core).wait()
                        if not turned:
                            left[k, core] = parts[k, core].T
                tile = jnp.concatenate([left[k, core] for k in group], axis=Z)
                dest[now, place:place + some] = nn(tile, right[...]).reshape(some, rows, -1)

    @pl.when(n == Z)
    def _():
        products(True)

    @pl.when((n >= 1) & (n < steps))
    def _():
        products(False)

    @pl.when(n >= 1)
    def _():
        copy(then).wait()
        color = color_of(n - 1, plan)
        for index, (split, _) in enumerate(plan):
            @pl.when(color == index)
            def _():
                for place in range(8):
                    z, y, x = place // 4, place // 2 % 2, place % 2
                    half, k = {'z': (z, 2 * y + x), 'y': (y, 2 * z + x), 'x': (x, 2 * z + y)}[split]
                    outs[2 * index + 1 - half][k] = mine[then, place] + came[then, place]

    @pl.when((n >= 1) & (n < steps - 1))
    def _():
        pl.semaphore_signal(free_sem, inc=1, device_id=other, device_id_type=mesh_id)


def pair_call(left, right, plan, tile, call_id):
    turned = left.ndim == 4
    rows = left.shape[2] if turned else LANES
    steps = sum(count for _, count in plan)
    out_specs, out_shape, edge = [], [], Z
    for _, count in plan:
        spec = pl.BlockSpec((4, rows, tile), lambda n, edge=edge, count=count: (Z, Z, jnp.clip(n - 1 - edge, Z, count - 1)))
        out_specs += [spec, spec]
        out_shape += [jax.ShapeDtypeStruct((4, rows, count * tile), F32)] * 2
        edge += count
    both = pltpu.VMEM((2, 8, rows, tile), F32)
    two = pltpu.SemaphoreType.DMA((2,))
    staging = [] if turned else [pltpu.VMEM((8, 2, MODEL, LANES), BF)]
    return pl.pallas_call(
        functools.partial(pair_kernel, plan, rows, turned), grid=(steps + 1,), name='pair',
        in_specs=[pl.BlockSpec(memory_space=pl.ANY), pl.BlockSpec((MODEL, tile), lambda n: (Z, jnp.minimum(n, steps - 1)))],
        out_specs=out_specs, out_shape=out_shape,
        scratch_shapes=[both, both, both, two, two, pltpu.SemaphoreType.REGULAR, *staging, pltpu.VMEM((8, 2, rows, MODEL), BF),
                        pltpu.SemaphoreType.DMA((8, 2))],
        cost_estimate=timed(16 * rows * steps * tile * 4096 / 9e8),
        compiler_params=pltpu.CompilerParams(vmem_limit_bytes=63 * 2**20, collective_id=call_id, has_side_effects=True),
    )(left, right)


def halve(keep, got, axis):
    return tuple(pick(keep, axis, k) + pick(got, axis, k) for k in (1, Z))


def weight_grad(left, right, plan, tile, call_id, flip=False):
    outs = pair_call(left, right, plan, tile, call_id)
    keeps, gots, fars = [], [], []
    for (split, _), send, keep in zip(plan, outs[::2], outs[1::2]):
        shape = (2, 2, *keep.shape[1:])
        got = swap(send, split).reshape(shape)
        send, keep = lax.optimization_barrier(halve(keep.reshape(shape), got, Z if split == 'y' else 1))
        got = swap(send, NEXT[split][Z])
        keeps.append(keep)
        gots.append(got)
        fars.append(swap(keep[1] + got[1], NEXT[split][1]))
    return final(keeps, gots, fars, flip)


def final_kernel(flip, *refs):
    count, edge = len(refs) // 3, Z
    for index in range(count):
        keep, got, far = refs[index:-1:count]
        total = (keep[Z] + got[Z] + far[...]) / 16
        cut = slice(edge, edge + total.shape[1])
        edge = cut.stop
        if flip:
            refs[-1][cut, :] = total.T
        else:
            refs[-1][:, cut] = total


def final(keeps, gots, fars, flip):
    shape = (fars[Z].shape[Z], sum(far.shape[1] for far in fars))
    shape = shape[::-1] if flip else shape
    two = [pl.BlockSpec((1, *far.shape), lambda n: (Z, Z, Z)) for far in fars]
    one = [pl.BlockSpec(far.shape, lambda n: (Z, Z)) for far in fars]
    return pl.pallas_call(
        functools.partial(final_kernel, flip), grid=(1,), name='final', in_specs=two + two + one,
        out_specs=pl.BlockSpec(shape, lambda n: (Z, Z)), out_shape=jax.ShapeDtypeStruct(shape, F32),
        cost_estimate=timed(4), compiler_params=ALL_VMEM)(*keeps, *gots, *fars)


def small_kernel(bits_ref, *refs):
    right = refs[2][...]
    for core in range(2):
        refs[3 + core][Z] = tn(refs[core][...], right)


def small_grad(bits, left, right):
    def column(core):
        return lambda k, m: (Z, ((k % 2) ^ m[Z]) * 8 + ((k // 2 % 2) ^ m[1]) * 4 + ((k // 4) ^ m[2]) * 2 + (core ^ m[3]))

    out = pl.BlockSpec((1, LANES, WIDE), lambda k, m: (k, Z, Z))
    grid_spec = pltpu.PrefetchScalarGridSpec(
        num_scalar_prefetch=1, grid=(8,),
        in_specs=[pl.BlockSpec((MODEL, LANES), column(core)) for core in range(2)] + [pl.BlockSpec((MODEL, WIDE), lambda k, m: (Z, Z))],
        out_specs=[out, out])
    keep, send = pl.pallas_call(small_kernel, grid_spec=grid_spec, name='small', out_shape=[jax.ShapeDtypeStruct((8, LANES, WIDE), F32)] * 2,
                                cost_estimate=timed(8), compiler_params=ALL_VMEM)(bits, left, left, right)
    for link in 'cxy':
        got, half = swap(send, link), keep.shape[Z] // 2
        send, keep = lax.optimization_barrier((keep[half:] + got[half:], keep[:half] + got[:half]))
    return (keep[Z] + swap(send, 'z')[Z]) / 16


def join_kernel(*refs):
    row = Z
    for chunk in range(Z, len(refs) - 1, 4):
        rows = slice(row, row + refs[chunk].shape[Z])
        row = rows.stop
        for color in range(2):
            total, far = refs[chunk + 2 * color:chunk + 2 * color + 2]
            refs[-1][rows, :, CHUNK * color:CHUNK * (color + 1)] = (total[...] + far[...]).astype(BF)


def join(parts):
    return pl.pallas_call(join_kernel, name='join', out_shape=jax.ShapeDtypeStruct((16, LANES, WIDE), BF),
                          cost_estimate=timed(4), compiler_params=ALL_VMEM)(*parts)


def gather_kv(kv, order):
    held = {Z: kv}
    for link in order:
        held.update({pos ^ BITS[link]: swap(tile, link) for pos, tile in list(held.items())})
    return [held[pos] for pos in range(8)]


def reduce_dkv(keep, send):
    got = swap(send, 'c')
    parts = []
    for color, (first, second) in enumerate((('x', 'y'), ('y', 'x'))):
        more = swap(keep[color, 1] + got[color, 1], first)
        send, total = lax.optimization_barrier(tuple(keep[color, Z, k] + got[color, Z, k] + more[k] for k in (1, Z)))
        parts += [total, swap(send, second)]
    return parts


CHUNKS = ((Z, 8), (8, 4), (12, 4))
PLAN_UP = (('z', 5), ('y', 3), ('x', 3))
PLAN_D = (('z', 4), ('y', 2), ('x', 2))


def solution(mesh):
    def per_device(x_loc, cot_loc, w_q, w_k, w_v, w_o, w_up, w_down):
        batch, seq, d_model = x_loc.shape
        tokens = batch * seq
        me = lax.axis_index('cp').astype(jnp.int32)
        me_one = me.reshape(1)
        bits = jnp.stack([lax.axis_index('dp').astype(jnp.int32), me >> 2, (me >> 1) & 1, me & 1])
        x2, cot2 = x_loc.reshape(tokens, d_model), cot_loc.reshape(tokens, d_model)
        w_q2, w_k2, w_v2, w_o2 = (w.transpose(1, 2, Z).reshape(-1, d_model) for w in (w_q, w_k, w_v, w_o))

        kvs = [kv.reshape(batch // 2, seq, -1) for kv in kv_call(x2, w_k2, w_v2)]
        gathered = [gather_kv(kvs[Z], 'xyc'), gather_kv(kvs[1], 'yxc')]
        q = mm(x2, w_q2, WIDE, Z, 2, SEQ).reshape(batch, seq, -1)
        grad_act = mm(cot2, w_down, WIDE, Z, 4, FF_TILE)

        o, lse_first = attn_fwd(me_one, q, gathered[Z], Z, batch)
        o, lse_second = attn_fwd(me_one, q, gathered[1], batch // 2, batch, o)
        lse = [lse_first, lse_second]
        o2 = o.reshape(tokens, -1)
        h = mm(o2, w_o2, WIDE, Z, 2, SEQ, False, x2)

        act_t, grad_u = ff_block(bits, h, w_up, grad_act)
        grad_w_up = weight_grad(h, grad_u, PLAN_UP, WIDE, Z)
        grad_w_down = weight_grad(act_t.reshape(8, 2, -1, tokens), cot2, PLAN_D, CHUNK, 1)
        grad_h = mm(grad_u, w_up, WIDE, Z, 4, WIDE, True, cot2)
        grad_o = mm(grad_h, w_o2, WIDE, Z, 2, SEQ).reshape(batch, seq, -1)

        grad_q, grad_kv = None, []
        for part, (first, count) in enumerate(CHUNKS):
            side, sub = first // 8, first % 8
            grad_q, keep, send = attn_bwd(me_one, q, grad_o, lse[side], gathered[side], first, sub, count, grad_q)
            grad_kv += reduce_dkv(keep, send)
            if part == Z:
                grad_w_o = weight_grad(grad_h, o2, PLAN_D, CHUNK, 2, True)
        grad_q2 = grad_q.reshape(tokens, -1)
        grad_w_q = weight_grad(x2, grad_q2, PLAN_D, CHUNK, 3, True)
        grad_kv2 = join(grad_kv).reshape(tokens, -1)
        grad_w_kv = small_grad(bits, x2, grad_kv2).reshape(-1, 4, 2, HALF)
        grad_x = None
        for part in range(2):
            grad_x = gx_call(grad_h, grad_q2, grad_kv2, w_q2, w_k2, w_v2, part, grad_x)
        return (grad_x.reshape(x_loc.shape), grad_w_q.reshape(32, HALF, -1).transpose(2, Z, 1), grad_w_kv[:, :, Z], grad_w_kv[:, :, 1],
                grad_w_o.reshape(32, HALF, -1).transpose(2, Z, 1), grad_w_up, grad_w_down)

    act_spec = P('dp', 'cp', None)
    rep_three, rep_two = P(None, None, None), P(None, None)
    grad_three, grad_two = P(('dp', 'cp'), None, None), P(('dp', 'cp'), None)
    return jax.shard_map(per_device, mesh=mesh,
                         in_specs=(act_spec, act_spec, rep_three, rep_three, rep_three, rep_three, rep_two, rep_two),
                         out_specs=(act_spec, grad_three, grad_three, grad_three, grad_three, grad_two, grad_two),
                         check_vma=False)
```

```python
import functools, math
import jax, jax.numpy as jnp
from jax import lax
from jax.experimental import pallas as pl
from jax.experimental.pallas import tpu as pltpu
from jax.sharding import PartitionSpec as P


BF, F32 = jnp.bfloat16, jnp.float32
NEG_BIG = -1e30
LANES, WIDE, MODEL, FF_TILE, FF_ROWS, SEQ, Z = 128, 512, 2048, 1408, 352, 1024, 0
HALF = 64
CHUNK = 256
HEADS = 2
NORM = True


def nt(a, b):
    return lax.dot_general(a, b, (((1,), (1,)), ((), ())), preferred_element_type=F32)


def tn(a, b):
    return lax.dot_general(a, b, (((Z,), (Z,)), ((), ())), preferred_element_type=F32)


def nn(a, b):
    return lax.dot_general(a, b, (((1,), (Z,)), ((), ())), preferred_element_type=F32)


def low_lanes(rows):
    return lax.broadcasted_iota(jnp.int32, (rows, LANES), 1) < HALF


def load_keys(me, kv_refs, keys, vals, head):
    low = low_lanes(LANES)
    for pos, ref in enumerate(kv_refs):
        dev = me ^ pos
        tile = ref[Z, :, LANES * head:LANES * (head + 1)]
        flipped = jnp.concatenate([tile[:, HALF:], tile[:, :HALF]], axis=1)
        k_two = jnp.where(low, tile, flipped)
        v_two = jnp.where(low, flipped, tile)
        first = pl.multiple_of(dev * HALF, HALF)
        second = pl.multiple_of((15 - dev) * HALF, HALF)
        keys[pl.ds(first, HALF), :] = k_two[:HALF]
        keys[pl.ds(second, HALF), :] = k_two[HALF:]
        vals[pl.ds(first, HALF), :] = v_two[:HALF]
        vals[pl.ds(second, HALF), :] = v_two[HALF:]


def spread_heads(rows):
    low = low_lanes(HALF)
    zero = jnp.zeros((HALF, LANES), BF)
    parts = []
    for pair in range(4):
        tile = rows[:, LANES * pair:LANES * (pair + 1)]
        parts += [jnp.where(low, tile, zero), jnp.where(low, zero, tile)]
    return jnp.concatenate(parts, axis=Z)


def gather_heads(cols, ref, base, lane):
    low = low_lanes(HALF)
    for pair in range(4):
        tile = cols[:, LANES * pair:LANES * (pair + 1)].T
        ref[Z, base:base + HALF, lane + LANES * pair:lane + LANES * (pair + 1)] = jnp.where(low, tile[:HALF], tile[HALF:]).astype(BF)


def tile_plan(me):
    late = me >= 4
    fifth_key = pl.multiple_of(jnp.where(late, CHUNK, 768), CHUNK)
    fifth_block = jnp.where(late, me, 15 - me)
    return late, [(Z, me, True, Z), (Z, 15 - me, False, 1), (CHUNK, 15 - me, False, 1),
                  (2 * CHUNK, 15 - me, True, 1), (fifth_key, fifth_block, True, 2)]


def lag():
    row = lax.broadcasted_iota(jnp.int32, (CHUNK, WIDE), Z)
    col = lax.broadcasted_iota(jnp.int32, (CHUNK, WIDE), 1)
    return row - (col & (HALF - 1))


def fwd_kernel(scale2, aliased, me_ref, q_ref, *refs):
    kv_refs = refs[:8]
    refs = refs[8 + (1 if aliased else Z):]
    o_ref, lse_ref, keys, vals = refs
    me = me_ref[Z]
    gap = lag()
    late, plan = tile_plan(me)

    def choose(one, two):
        return [one, two, jnp.where(late, one, two)]

    def split(parts):
        zero = jnp.zeros_like(parts[4])
        return parts[Z] + jnp.where(late, parts[4], zero), parts[1] + parts[2] + parts[3] + jnp.where(late, zero, parts[4])

    class Head:
        pass

    heads = []
    for head in range(HEADS):
        x = Head()
        load_keys(me, kv_refs, keys.at[head], vals.at[head], head)
        lanes = slice(WIDE * head, WIDE * (head + 1))
        q_tile = q_ref[Z, :, lanes]
        x.q = choose(spread_heads(q_tile[:HALF]), spread_heads(q_tile[HALF:]))
        x.scores, x.tops, x.exps, x.sums, x.outs = [], [], [], [], []
        heads.append(x)

    def score(head, i):
        x = heads[head]
        start, block, masked, which = plan[i]
        s = nt(keys[head, pl.ds(start, CHUNK), :], x.q[which])
        if masked:
            s = jnp.where(gap <= block * HALF - start, s, NEG_BIG)
        x.scores.append(s)
        x.tops.append(jnp.max(s, axis=Z, keepdims=True))

    def top(head):
        x = heads[head]
        t = x.tops
        top_b = jnp.maximum(jnp.maximum(t[1], t[2]), t[3])
        top_a = jnp.where(late, jnp.maximum(t[Z], t[4]), t[Z]) * scale2
        top_b = jnp.where(late, top_b, jnp.maximum(top_b, t[4])) * scale2
        x.top = choose(top_a, top_b)

    def expo(head, i):
        x = heads[head]
        e = jnp.exp2(x.scores[i] * scale2 - x.top[plan[i][3]])
        x.exps.append(e if NORM else e.astype(BF))
        x.sums.append(jnp.sum(e, axis=Z, keepdims=True))

    def total(head):
        x = heads[head]
        sum_a, sum_b = split(x.sums)
        lse_ref[head, Z:1, :] = x.top[Z] + jnp.log2(sum_a)
        lse_ref[head, 1:2, :] = x.top[1] + jnp.log2(sum_b)
        x.inv = choose(1.0 / sum_a, 1.0 / sum_b)

    def value(head, i):
        x = heads[head]
        p = (x.exps[i] * x.inv[plan[i][3]]).astype(BF) if NORM else x.exps[i]
        x.outs.append(tn(vals[head, pl.ds(plan[i][Z], CHUNK), :], p))

    def finish(head):
        x = heads[head]
        out_a, out_b = split(x.outs)
        if not NORM:
            out_a, out_b = out_a * x.inv[Z], out_b * x.inv[1]
        gather_heads(out_a, o_ref, Z, WIDE * head)
        gather_heads(out_b, o_ref, HALF, WIDE * head)

    n = len(plan)
    for head in range(HEADS + 2):
        for i in range(n):
            if head < HEADS:
                score(head, i)
            if Z <= head - 1 < HEADS:
                if i == Z:
                    top(head - 1)
                expo(head - 1, i)
            if Z <= head - 2 < HEADS:
                if i == Z:
                    total(head - 2)
                value(head - 2, i)
        if Z <= head - 2 < HEADS:
            finish(head - 2)


def bwd_kernel(scale, scale2, aliased, me_ref, q_ref, g_ref, lse_ref, *refs):
    kv_refs = refs[:8]
    refs = refs[8 + (1 if aliased else Z):]
    dq_ref, keep_ref, send_ref, keys, vals, grads = refs
    me = me_ref[Z]
    gap = lag()
    late, plan = tile_plan(me)
    low = low_lanes(CHUNK)

    def choose(one, two):
        return [one, two, jnp.where(late, one, two)]

    def split(parts):
        zero = jnp.zeros_like(parts[4])
        return parts[Z] + jnp.where(late, parts[4], zero), parts[1] + parts[2] + parts[3] + jnp.where(late, zero, parts[4])

    class Head:
        pass

    heads = []
    for head in range(HEADS):
        x = Head()
        load_keys(me, kv_refs, keys.at[head], vals.at[head], head)
        lanes = slice(WIDE * head, WIDE * (head + 1))
        q_tile, g_tile = q_ref[Z, :, lanes], g_ref[Z, :, lanes]
        x.q = choose(spread_heads(q_tile[:HALF]), spread_heads(q_tile[HALF:]))
        x.g = choose(spread_heads(g_tile[:HALF]), spread_heads(g_tile[HALF:]))
        x.lse = choose(lse_ref[head, Z:1, :], lse_ref[head, 1:2, :])
        x.probs, x.dprobs, x.deltas, x.dqs, x.dks, x.dvs = [], [], [], [], [], []
        heads.append(x)

    def prob(head, i):
        x = heads[head]
        start, block, masked, which = plan[i]
        s = nt(keys[head, pl.ds(start, CHUNK), :], x.q[which])
        if masked:
            s = jnp.where(gap <= block * HALF - start, s, NEG_BIG)
        p = jnp.exp2(s * scale2 - x.lse[which])
        dp = nt(vals[head, pl.ds(start, CHUNK), :], x.g[which]).astype(BF)
        x.probs.append(p)
        x.dprobs.append(dp)
        x.deltas.append(jnp.sum(p * dp.astype(F32), axis=Z, keepdims=True))

    def delta(head):
        x = heads[head]
        x.delta = choose(*split(x.deltas))

    def grad(head, i):
        x = heads[head]
        start, _, _, which = plan[i]
        p, dp = x.probs[i], x.dprobs[i]
        ds = (p * (dp.astype(F32) - x.delta[which])).astype(BF)
        x.dvs.append(nn(p.astype(BF), x.g[which]))
        x.dks.append(nn(ds, x.q[which]))
        x.dqs.append(tn(keys[head, pl.ds(start, CHUNK), :], ds))

    def finish(head):
        x = heads[head]
        dq_a, dq_b = split(x.dqs)
        gather_heads(dq_a * scale, dq_ref, Z, WIDE * head)
        gather_heads(dq_b * scale, dq_ref, HALF, WIDE * head)
        zero = jnp.zeros_like(x.dks[4])

        def by_chunk(parts):
            return [parts[Z] + parts[1], parts[2] + jnp.where(late, parts[4], zero), parts[3],
                    jnp.where(late, zero, parts[4])]

        for chunk, (dk, dv) in enumerate(zip(by_chunk(x.dks), by_chunk(x.dvs))):
            dk = (dk + pltpu.roll(dk, HALF, 1)) * scale
            dv = dv + pltpu.roll(dv, HALF, 1)
            both = jnp.where(low, dk, dv)
            for sub in range(4):
                block = 4 * chunk + sub
                dev, base = (block, Z) if block < 8 else (15 - block, HALF)
                grads[dev ^ me, base:base + HALF, LANES * head:LANES * (head + 1)] = both[sub * HALF:(sub + 1) * HALF]

    n = len(plan)
    for head in range(HEADS + 1):
        for i in range(n):
            if head < HEADS:
                prob(head, i)
            if head >= 1:
                if i == Z:
                    delta(head - 1)
                grad(head - 1, i)
        if head >= 1:
            finish(head - 1)
    for one in range(2):
        for two in range(2):
            slot = jnp.where(pl.program_id(1) == Z, 2 * two + one, 2 * one + two)
            keep_ref[Z, one, two, Z] = grads[2 * slot]
            send_ref[Z, one, two, Z] = grads[2 * slot + 1]


def attn_fwd(me, q, kvs, first, total, o_prev=None):
    count = kvs[Z].shape[Z]
    scale2 = 0.125 * math.log2(math.e)
    aliased = o_prev is not None
    row = lambda b, g, m: (first + b, Z, g)
    kv_spec = pl.BlockSpec((1, LANES, LANES * HEADS), lambda b, g, m: (b, Z, g))
    grid_spec = pltpu.PrefetchScalarGridSpec(
        num_scalar_prefetch=1, grid=(count, 4 // HEADS),
        in_specs=[pl.BlockSpec((1, LANES, WIDE * HEADS), row)] + [kv_spec] * 8 + ([pl.BlockSpec(memory_space=pl.ANY)] if aliased else []),
        out_specs=[pl.BlockSpec((1, LANES, WIDE * HEADS), row), pl.BlockSpec((HEADS, 2, WIDE), lambda b, g, m: (b * (4 // HEADS) + g, Z, Z))],
        scratch_shapes=[pltpu.VMEM((HEADS, SEQ, LANES), BF), pltpu.VMEM((HEADS, SEQ, LANES), BF)])
    return pl.pallas_call(
        functools.partial(fwd_kernel, scale2, aliased), grid_spec=grid_spec, name='attn_fwd',
        out_shape=[jax.ShapeDtypeStruct((total, LANES, MODEL), BF), jax.ShapeDtypeStruct((count * 4, 2, WIDE), F32)],
        input_output_aliases={10: Z} if aliased else {},
        cost_estimate=timed(6 * count),
        compiler_params=ALL_VMEM,
    )(me, q, *kvs, *([o_prev] if aliased else []))


def attn_bwd(me, q, g, lse, kvs, first, sub, count, dq_prev=None):
    total = q.shape[Z]
    scale = 0.125
    scale2 = scale * math.log2(math.e)
    aliased = dq_prev is not None
    row = lambda b, h, m: (first + b, Z, h)
    kv_spec = pl.BlockSpec((1, LANES, LANES * HEADS), lambda b, h, m: (sub + b, Z, h))
    part = pl.BlockSpec((1, 2, 2, 1, LANES, CHUNK), lambda b, h, m: (h, Z, Z, b, Z, Z))
    part_shape = jax.ShapeDtypeStruct((2, 2, 2, count, LANES, CHUNK), F32)
    grid_spec = pltpu.PrefetchScalarGridSpec(
        num_scalar_prefetch=1, grid=(count, 4 // HEADS),
        in_specs=[pl.BlockSpec((1, LANES, WIDE * HEADS), row), pl.BlockSpec((1, LANES, WIDE * HEADS), row),
                  pl.BlockSpec((HEADS, 2, WIDE), lambda b, h, m: ((sub + b) * (4 // HEADS) + h, Z, Z))] + [kv_spec] * 8
        + ([pl.BlockSpec(memory_space=pl.ANY)] if aliased else []),
        out_specs=[pl.BlockSpec((1, LANES, WIDE * HEADS), row), part, part],
        scratch_shapes=[pltpu.VMEM((HEADS, SEQ, LANES), BF), pltpu.VMEM((HEADS, SEQ, LANES), BF), pltpu.VMEM((8, LANES, LANES * HEADS), F32)])
    return pl.pallas_call(
        functools.partial(bwd_kernel, scale, scale2, aliased), grid_spec=grid_spec, name='attn_bwd',
        out_shape=[jax.ShapeDtypeStruct((total, LANES, MODEL), BF)] + [part_shape] * 2,
        input_output_aliases={12: Z} if aliased else {},
        cost_estimate=timed(10 * count),
        compiler_params=ALL_VMEM,
    )(me, q, g, lse, *kvs, *([dq_prev] if aliased else []))


BITS = {'c': 1, 'x': 2, 'y': 4}
ALL_VMEM = pltpu.CompilerParams(vmem_limit_bytes=63 * 2**20)
FF_PARAMS = pltpu.CompilerParams(vmem_limit_bytes=63 * 2**20)
NEXT = {'x': ('y', 'z'), 'y': ('z', 'x'), 'z': ('x', 'y')}


def swap(values, link):
    if link == 'z':
        return lax.ppermute(values, 'dp', [(Z, 1), (1, Z)])
    return lax.ppermute(values, 'cp', [(i, i ^ BITS[link]) for i in range(8)])


def pick(values, axis, index):
    return lax.index_in_dim(values, index, axis, keepdims=False)


def timed(micros):
    return pl.CostEstimate(flops=int(micros * 9e8), bytes_accessed=1 << 20, transcendentals=Z)


def mm_kernel(product, added, x_ref, w_ref, *refs):
    total = product(x_ref[...], w_ref[...])
    if added:
        total = total + refs[Z][...].astype(F32)
    refs[-1][...] = total.astype(refs[-1].dtype)


def mm(x, w, rows, first, count, width, flip=True, added=None, dtype=BF):
    total, depth = x.shape
    tile = pl.BlockSpec((rows, width), lambda n, t: (t, n))
    w_spec = pl.BlockSpec((width, depth), lambda n, t: (first + n, Z)) if flip else pl.BlockSpec(
        (depth, width), lambda n, t: (Z, first + n))
    return pl.pallas_call(
        functools.partial(mm_kernel, nt if flip else nn, added is not None), grid=(count, total // rows), name='mm',
        in_specs=[pl.BlockSpec((rows, depth), lambda n, t: (t, Z)), w_spec] + ([tile] if added is not None else []),
        out_specs=tile, out_shape=jax.ShapeDtypeStruct((total, count * width), dtype),
        cost_estimate=timed(total * count * width * depth * 2 / 9e8),
        compiler_params=ALL_VMEM)(x, w, *([added] if added is not None else []))


def join_kv(k_ref, v_ref, both):
    @pl.when(pl.program_id(Z) == Z)
    def _():
        for head in range(4):
            both[LANES * head:LANES * head + HALF, :] = k_ref[HALF * head:HALF * head + HALF, :]
            both[LANES * head + HALF:LANES * head + LANES, :] = v_ref[HALF * head:HALF * head + HALF, :]


def kv_kernel(x_ref, k_ref, v_ref, low_ref, high_ref, both):
    join_kv(k_ref, v_ref, both)
    value = nt(x_ref[...], both[...]).astype(BF)
    for index, ref in enumerate((low_ref, high_ref)):
        @pl.when(pl.program_id(Z) // 2 == index)
        def _():
            ref[...] = value


def kv_call(x, w_k, w_v):
    rows, (total, depth) = WIDE, x.shape
    whole = pl.BlockSpec((CHUNK, depth), lambda t: (Z, Z), pipeline_mode=pl.Buffered(1))
    return pl.pallas_call(
        kv_kernel, grid=(total // rows,), name='kv',
        in_specs=[pl.BlockSpec((rows, depth), lambda t: (t, Z)), whole, whole],
        out_specs=[pl.BlockSpec((rows, WIDE), lambda t: (jnp.minimum(t, 1), Z)), pl.BlockSpec((rows, WIDE), lambda t: (jnp.maximum(t - 2, Z), Z))],
        out_shape=[jax.ShapeDtypeStruct((total // 2, WIDE), BF)] * 2,
        scratch_shapes=[pltpu.VMEM((WIDE, depth), BF)], cost_estimate=timed(9), compiler_params=ALL_VMEM)(x, w_k, w_v)


def gx_kernel(h_ref, q_ref, g_ref, w_ref, k_ref, v_ref, *refs):
    out_ref, both = refs[-2:]
    join_kv(k_ref, v_ref, both)
    total = nn(q_ref[...], w_ref[...]) + nn(g_ref[...], both[...])
    out_ref[...] = (h_ref[...].astype(F32) + total).astype(BF)


def gx_call(grad_h, grad_q, grad_kv, w_q, w_k, w_v, half, prev=None):
    rows, (total, depth) = WIDE, grad_h.shape
    width = depth // 2
    aliased = prev is not None
    tile = pl.BlockSpec((rows, width), lambda t: (t, half))
    once = lambda count: pl.BlockSpec((count, width), lambda t: (Z, half), pipeline_mode=pl.Buffered(1))
    return pl.pallas_call(
        gx_kernel, grid=(total // rows,), name='gx',
        in_specs=[tile, pl.BlockSpec((rows, depth), lambda t: (t, Z)), pl.BlockSpec((rows, WIDE), lambda t: (t, Z)), once(depth), once(CHUNK),
                  once(CHUNK)] + ([pl.BlockSpec(memory_space=pl.ANY)] if aliased else []),
        out_specs=tile, out_shape=jax.ShapeDtypeStruct((total, depth), BF), scratch_shapes=[pltpu.VMEM((WIDE, width), BF)],
        input_output_aliases={6: Z} if aliased else {}, cost_estimate=timed(14), compiler_params=ALL_VMEM,
    )(grad_h, grad_q, grad_kv, w_q, w_k, w_v, *([prev] if aliased else []))


def ff_kernel(bits_ref, h_ref, w_ref, ga_ref, at_ref, gu_ref, held, turned):
    root = math.sqrt(2.0 / math.pi)
    width = w_ref.shape[1]
    for lo in range(Z, width, CHUNK):
        cut = slice(lo, min(lo + CHUNK, width))
        u = held[:, cut]
        held[:, cut] = nn(h_ref[...], w_ref[:, cut])
        rise = (root * 0.044715) * (u * u)
        t = jnp.tanh(u * (root + rise))
        up, down, half_u = 1.0 + t, 1.0 - t, 0.5 * u
        slope = up * (0.5 + (half_u * down) * (root + 3.0 * rise))
        gu_ref[:, cut] = (ga_ref[:, cut].astype(F32) * slope).astype(BF)
        turned[cut, :] = (half_u * up).T.astype(BF)
    for x in range(2):
        for c in range(2):
            lo = (2 * x + c) * FF_ROWS
            at_ref[Z, Z, x ^ bits_ref[2], c ^ bits_ref[3]] = turned[lo:lo + FF_ROWS, :]


def ff_block(bits, h, w_up, ga):
    tokens, width, rows = MODEL, FF_TILE, WIDE
    per = tokens // rows
    steps = 4 * per
    now = lambda i: jnp.minimum(i, steps - 1)
    then = lambda i: jnp.maximum(i - 1, Z)
    grid_spec = pltpu.PrefetchScalarGridSpec(
        num_scalar_prefetch=1, grid=(steps + 1,),
        in_specs=[pl.BlockSpec((rows, MODEL), lambda i, m: (now(i) % per, Z)),
                  pl.BlockSpec((MODEL, width), lambda i, m: (Z, now(i) // per)),
                  pl.BlockSpec((rows, width), lambda i, m: (then(i) % per, then(i) // per))],
        out_specs=[pl.BlockSpec((1, 1, 2, 2, FF_ROWS, rows), lambda i, m: ((then(i) // per // 2) ^ m[Z], (then(i) // per % 2) ^ m[1], Z, Z, Z, then(i) % per)),
                   pl.BlockSpec((rows, width), lambda i, m: (then(i) % per, then(i) // per))],
        scratch_shapes=[pltpu.VMEM((rows, width), F32), pltpu.VMEM((width, rows), BF)])
    return pl.pallas_call(
        ff_kernel, grid_spec=grid_spec, name='ff_block',
        out_shape=[jax.ShapeDtypeStruct((2, 2, 2, 2, FF_ROWS, tokens), BF), jax.ShapeDtypeStruct((tokens, 5632), BF)],
        cost_estimate=timed(60), compiler_params=FF_PARAMS)(bits, h, w_up, ga)


def color_of(n, plan):
    edge, color = Z, Z
    for _, count in plan[:-1]:
        edge += count
        color = color + (n >= edge).astype(jnp.int32)
    return color


def pair_kernel(plan, rows, turned, *refs):
    n, steps = pl.program_id(Z), sum(count for _, count in plan)
    count = len(plan)
    if turned:
        left, refs = refs[Z], refs[1:]
    else:
        source, refs, (parts, left, load_sem) = refs[Z], refs[1:-3], refs[-3:]
    me = lax.axis_index('cp')
    bits = (lax.axis_index('dp'), me // 4, (me // 2) % 2, me % 2)

    def load(place, core):
        flips = (place // 4, place // 2 % 2, place % 2, core)
        block = sum((1 - bit if flip else bit) * weight for bit, flip, weight in zip(bits, flips, (8, 4, 2, 1)))
        columns = pl.ds(pl.multiple_of(block * LANES, LANES), LANES)
        return pltpu.make_async_copy(source.at[:, columns], parts.at[place, core], load_sem.at[place, core])

    right, outs = refs[Z], refs[1:1 + 2 * count]
    mine, sent, came, send_sem, recv_sem, free_sem = refs[1 + 2 * count:]
    other = {'cp': me + 1 - 2 * (me % 2)}
    mesh_id = pl.DeviceIdType.MESH
    now, then = n % 2, (n + 1) % 2

    def copy(slot):
        return pltpu.make_async_remote_copy(src_ref=sent.at[slot], dst_ref=came.at[slot], send_sem=send_sem.at[slot],
                                            recv_sem=recv_sem.at[slot], device_id=other, device_id_type=mesh_id)

    @pl.when(n == Z)
    def _():
        for core in () if turned else (1, Z):
            for place in range(8):
                load(place, core).start()
        barrier = pltpu.get_barrier_semaphore()
        pl.semaphore_signal(barrier, inc=1, device_id=other, device_id_type=mesh_id)
        pl.semaphore_wait(barrier, 1)

    @pl.when(n >= 3)
    def _():
        pl.semaphore_wait(free_sem, 1)

    @pl.when(n >= 1)
    def _():
        copy(then).start()

    def products(first):
        some = 1 if turned else 4
        for core, dest in ((1, sent), (Z, mine)):
            for place in range(Z, 8, some):
                group = range(place, place + some)
                for k in group if first else ():
                    load(k, core).wait()
                    left[k, core] = parts[k, core].T
                tile = jnp.concatenate([left[k, core] for k in group], axis=Z)
                dest[now, place:place + some] = nn(tile, right[...]).reshape(some, rows, -1)

    if not turned:
        @pl.when(n == Z)
        def _():
            products(True)

    @pl.when((n >= (Z if turned else 1)) & (n < steps))
    def _():
        products(False)

    @pl.when(n >= 1)
    def _():
        copy(then).wait()
        color = color_of(n - 1, plan)
        for index, (split, _) in enumerate(plan):
            @pl.when(color == index)
            def _():
                for place in range(8):
                    z, y, x = place // 4, place // 2 % 2, place % 2
                    half, k = {'z': (z, 2 * y + x), 'y': (y, 2 * z + x), 'x': (x, 2 * z + y)}[split]
                    outs[2 * index + 1 - half][k] = mine[then, place] + came[then, place]

    @pl.when((n >= 1) & (n < steps - 1))
    def _():
        pl.semaphore_signal(free_sem, inc=1, device_id=other, device_id_type=mesh_id)


def pair_call(left, right, plan, tile, call_id):
    turned = left.ndim == 4
    rows = left.shape[2] if turned else LANES
    steps = sum(count for _, count in plan)
    out_specs, out_shape, edge = [], [], Z
    for _, count in plan:
        spec = pl.BlockSpec((4, rows, tile), lambda n, edge=edge, count=count: (Z, Z, jnp.clip(n - 1 - edge, Z, count - 1)))
        out_specs += [spec, spec]
        out_shape += [jax.ShapeDtypeStruct((4, rows, count * tile), F32)] * 2
        edge += count
    both = pltpu.VMEM((2, 8, rows, tile), F32)
    two = pltpu.SemaphoreType.DMA((2,))
    staging = [] if turned else [pltpu.VMEM((8, 2, MODEL, LANES), BF), pltpu.VMEM((8, 2, rows, MODEL), BF), pltpu.SemaphoreType.DMA((8, 2))]
    whole = pl.BlockSpec((8, 2, rows, MODEL), lambda n: (Z, Z, Z, Z), pipeline_mode=pl.Buffered(1))
    return pl.pallas_call(
        functools.partial(pair_kernel, plan, rows, turned), grid=(steps + 1,), name='pair',
        in_specs=[whole if turned else pl.BlockSpec(memory_space=pl.ANY),
                  pl.BlockSpec((MODEL, tile), lambda n: (Z, jnp.minimum(n, steps - 1)))],
        out_specs=out_specs, out_shape=out_shape,
        scratch_shapes=[both, both, both, two, two, pltpu.SemaphoreType.REGULAR, *staging],
        cost_estimate=timed(16 * rows * steps * tile * 4096 / 9e8),
        compiler_params=pltpu.CompilerParams(vmem_limit_bytes=63 * 2**20, collective_id=call_id, has_side_effects=True),
    )(left, right)


def halve(keep, got, axis):
    return tuple(pick(keep, axis, k) + pick(got, axis, k) for k in (1, Z))


def weight_grad(left, right, plan, tile, call_id, flip=False):
    outs = pair_call(left, right, plan, tile, call_id)
    keeps, gots, fars = [], [], []
    for (split, _), send, keep in zip(plan, outs[::2], outs[1::2]):
        shape = (2, 2, *keep.shape[1:])
        got = swap(send, split).reshape(shape)
        send, keep = lax.optimization_barrier(halve(keep.reshape(shape), got, Z if split == 'y' else 1))
        got = swap(send, NEXT[split][Z])
        keeps.append(keep)
        gots.append(got)
        fars.append(swap(keep[1] + got[1], NEXT[split][1]))
    return final(keeps, gots, fars, flip)


def final_kernel(flip, *refs):
    count, edge = len(refs) // 3, Z
    for index in range(count):
        keep, got, far = refs[index:-1:count]
        total = (keep[Z] + got[Z] + far[...]) / 16
        cut = slice(edge, edge + total.shape[1])
        edge = cut.stop
        if flip:
            refs[-1][cut, :] = total.T
        else:
            refs[-1][:, cut] = total


def final(keeps, gots, fars, flip):
    shape = (fars[Z].shape[Z], sum(far.shape[1] for far in fars))
    shape = shape[::-1] if flip else shape
    two = [pl.BlockSpec((1, *far.shape), lambda n: (Z, Z, Z)) for far in fars]
    one = [pl.BlockSpec(far.shape, lambda n: (Z, Z)) for far in fars]
    return pl.pallas_call(
        functools.partial(final_kernel, flip), grid=(1,), name='final', in_specs=two + two + one,
        out_specs=pl.BlockSpec(shape, lambda n: (Z, Z)), out_shape=jax.ShapeDtypeStruct(shape, F32),
        cost_estimate=timed(4), compiler_params=ALL_VMEM)(*keeps, *gots, *fars)


def small_kernel(bits_ref, *refs):
    right = refs[2][...]
    for core in range(2):
        refs[3 + core][Z] = tn(refs[core][...], right)


def small_grad(bits, left, right):
    def column(core):
        return lambda k, m: (Z, ((k % 2) ^ m[Z]) * 8 + ((k // 4) ^ m[1]) * 4 + ((k // 2 % 2) ^ m[2]) * 2 + (core ^ m[3]))

    out = pl.BlockSpec((1, LANES, WIDE), lambda k, m: (k, Z, Z))
    grid_spec = pltpu.PrefetchScalarGridSpec(
        num_scalar_prefetch=1, grid=(8,),
        in_specs=[pl.BlockSpec((MODEL, LANES), column(core)) for core in range(2)] + [pl.BlockSpec((MODEL, WIDE), lambda k, m: (Z, Z))],
        out_specs=[out, out])
    keep, send = pl.pallas_call(small_kernel, grid_spec=grid_spec, name='small', out_shape=[jax.ShapeDtypeStruct((8, LANES, WIDE), F32)] * 2,
                                cost_estimate=timed(8), compiler_params=ALL_VMEM)(bits, left, left, right)
    for link in 'cyx':
        got, half = swap(send, link), keep.shape[Z] // 2
        send, keep = lax.optimization_barrier((keep[half:] + got[half:], keep[:half] + got[:half]))
    return (keep[Z] + swap(send, 'z')[Z]) / 16


def join_kernel(*refs):
    row = Z
    for chunk in range(Z, len(refs) - 1, 4):
        rows = slice(row, row + refs[chunk].shape[Z])
        row = rows.stop
        for color in range(2):
            total, far = refs[chunk + 2 * color:chunk + 2 * color + 2]
            refs[-1][rows, :, CHUNK * color:CHUNK * (color + 1)] = (total[...] + far[...]).astype(BF)


def join(parts):
    return pl.pallas_call(join_kernel, name='join', out_shape=jax.ShapeDtypeStruct((16, LANES, WIDE), BF),
                          cost_estimate=timed(4), compiler_params=ALL_VMEM)(*parts)


def gather_kv(kv, order):
    held = {Z: kv}
    for link in order:
        held.update({pos ^ BITS[link]: swap(tile, link) for pos, tile in list(held.items())})
    return [held[pos] for pos in range(8)]


def reduce_dkv(keep, send):
    got = swap(send, 'c')
    parts = []
    for color, (first, second) in enumerate((('x', 'y'), ('y', 'x'))):
        more = swap(keep[color, 1] + got[color, 1], first)
        send, total = lax.optimization_barrier(tuple(keep[color, Z, k] + got[color, Z, k] + more[k] for k in (1, Z)))
        parts += [total, swap(send, second)]
    return parts


CHUNKS = ((Z, 8), (8, 4), (12, 4))
PLAN_UP = (('z', 5), ('y', 4), ('x', 2))
PLAN_D = (('z', 4), ('y', 2), ('x', 2))
PLAN_Q = (('z', 3), ('y', 3), ('x', 2))


def solution(mesh):
    def per_device(x_loc, cot_loc, w_q, w_k, w_v, w_o, w_up, w_down):
        batch, seq, d_model = x_loc.shape
        tokens = batch * seq
        me = lax.axis_index('cp').astype(jnp.int32)
        me_one = me.reshape(1)
        bits = jnp.stack([lax.axis_index('dp').astype(jnp.int32), me >> 2, (me >> 1) & 1, me & 1])
        x2, cot2 = x_loc.reshape(tokens, d_model), cot_loc.reshape(tokens, d_model)
        w_q2, w_k2, w_v2, w_o2 = (w.transpose(1, 2, Z).reshape(-1, d_model) for w in (w_q, w_k, w_v, w_o))

        kvs = [kv.reshape(batch // 2, seq, -1) for kv in kv_call(x2, w_k2, w_v2)]
        gathered = [gather_kv(kvs[Z], 'xyc'), gather_kv(kvs[1], 'yxc')]
        q = mm(x2, w_q2, WIDE, Z, 2, SEQ).reshape(batch, seq, -1)
        grad_act = mm(cot2, w_down, WIDE, Z, 4, FF_TILE)

        o, lse_first = attn_fwd(me_one, q, gathered[Z], Z, batch)
        o, lse_second = attn_fwd(me_one, q, gathered[1], batch // 2, batch, o)
        lse = [lse_first, lse_second]
        o2 = o.reshape(tokens, -1)
        h = mm(o2, w_o2, WIDE, Z, 2, SEQ, False, x2)

        act_t, grad_u = ff_block(bits, h, w_up, grad_act)
        grad_w_up = weight_grad(h, grad_u, PLAN_UP, WIDE, Z)
        grad_w_down = weight_grad(act_t.reshape(8, 2, -1, tokens), cot2, PLAN_D, CHUNK, 1)
        grad_h = mm(grad_u, w_up, WIDE, Z, 4, WIDE, True, cot2)
        grad_o = mm(grad_h, w_o2, WIDE, Z, 2, SEQ).reshape(batch, seq, -1)

        grad_q, grad_kv = None, []
        for part, (first, count) in enumerate(CHUNKS):
            side, sub = first // 8, first % 8
            grad_q, keep, send = attn_bwd(me_one, q, grad_o, lse[side], gathered[side], first, sub, count, grad_q)
            grad_kv += reduce_dkv(keep, send)
            if part == Z:
                grad_w_o = weight_grad(grad_h, o2, PLAN_D, CHUNK, 2, True)
        grad_q2 = grad_q.reshape(tokens, -1)
        grad_w_q = weight_grad(x2, grad_q2, PLAN_Q, CHUNK, 3, True)
        grad_kv2 = join(grad_kv).reshape(tokens, -1)
        grad_w_kv = small_grad(bits, x2, grad_kv2).reshape(-1, 4, 2, HALF)
        grad_x = None
        for part in range(2):
            grad_x = gx_call(grad_h, grad_q2, grad_kv2, w_q2, w_k2, w_v2, part, grad_x)
        return (grad_x.reshape(x_loc.shape), grad_w_q.reshape(32, HALF, -1).transpose(2, Z, 1), grad_w_kv[:, :, Z], grad_w_kv[:, :, 1],
                grad_w_o.reshape(32, HALF, -1).transpose(2, Z, 1), grad_w_up, grad_w_down)

    act_spec = P('dp', 'cp', None)
    rep_three, rep_two = P(None, None, None), P(None, None)
    grad_three, grad_two = P(('dp', 'cp'), None, None), P(('dp', 'cp'), None)
    return jax.shard_map(per_device, mesh=mesh,
                         in_specs=(act_spec, act_spec, rep_three, rep_three, rep_three, rep_three, rep_two, rep_two),
                         out_specs=(act_spec, grad_three, grad_three, grad_three, grad_three, grad_two, grad_two),
                         check_vma=False)
```

```python
import functools, math
import jax, jax.numpy as jnp
from jax import lax
from jax.experimental import pallas as pl
from jax.experimental.pallas import tpu as pltpu
from jax.sharding import PartitionSpec as P


BF, F32 = jnp.bfloat16, jnp.float32
NEG_BIG = -1e30
LANES, WIDE, MODEL, FF_TILE, FF_ROWS, SEQ, Z = 128, 512, 2048, 1408, 352, 1024, 0
HALF = 64
CHUNK = 256
HEADS = 2
NORM = True


def nt(a, b):
    return lax.dot_general(a, b, (((1,), (1,)), ((), ())), preferred_element_type=F32)


def tn(a, b):
    return lax.dot_general(a, b, (((Z,), (Z,)), ((), ())), preferred_element_type=F32)


def nn(a, b):
    return lax.dot_general(a, b, (((1,), (Z,)), ((), ())), preferred_element_type=F32)


def low_lanes(rows):
    return lax.broadcasted_iota(jnp.int32, (rows, LANES), 1) < HALF


def load_keys(me, kv_refs, keys, vals, head):
    low = low_lanes(LANES)
    for pos, ref in enumerate(kv_refs):
        dev = me ^ pos
        tile = ref[Z, :, LANES * head:LANES * (head + 1)]
        flipped = jnp.concatenate([tile[:, HALF:], tile[:, :HALF]], axis=1)
        k_two = jnp.where(low, tile, flipped)
        v_two = jnp.where(low, flipped, tile)
        first = pl.multiple_of(dev * HALF, HALF)
        second = pl.multiple_of((15 - dev) * HALF, HALF)
        keys[pl.ds(first, HALF), :] = k_two[:HALF]
        keys[pl.ds(second, HALF), :] = k_two[HALF:]
        vals[pl.ds(first, HALF), :] = v_two[:HALF]
        vals[pl.ds(second, HALF), :] = v_two[HALF:]


def spread_heads(rows):
    low = low_lanes(HALF)
    zero = jnp.zeros((HALF, LANES), BF)
    parts = []
    for pair in range(4):
        tile = rows[:, LANES * pair:LANES * (pair + 1)]
        parts += [jnp.where(low, tile, zero), jnp.where(low, zero, tile)]
    return jnp.concatenate(parts, axis=Z)


def gather_heads(cols, ref, base, lane):
    low = low_lanes(HALF)
    for pair in range(4):
        tile = cols[:, LANES * pair:LANES * (pair + 1)].T
        ref[Z, base:base + HALF, lane + LANES * pair:lane + LANES * (pair + 1)] = jnp.where(low, tile[:HALF], tile[HALF:]).astype(BF)


def tile_plan(me):
    late = me >= 4
    fifth_key = pl.multiple_of(jnp.where(late, CHUNK, 768), CHUNK)
    fifth_block = jnp.where(late, me, 15 - me)
    return late, [(Z, me, True, Z), (Z, 15 - me, False, 1), (CHUNK, 15 - me, False, 1),
                  (2 * CHUNK, 15 - me, True, 1), (fifth_key, fifth_block, True, 2)]


def lag():
    row = lax.broadcasted_iota(jnp.int32, (CHUNK, WIDE), Z)
    col = lax.broadcasted_iota(jnp.int32, (CHUNK, WIDE), 1)
    return row - (col & (HALF - 1))


def fwd_kernel(scale2, aliased, me_ref, q_ref, *refs):
    kv_refs = refs[:8]
    refs = refs[8 + (1 if aliased else Z):]
    o_ref, lse_ref, keys, vals = refs
    me = me_ref[Z]
    gap = lag()
    late, plan = tile_plan(me)

    def choose(one, two):
        return [one, two, jnp.where(late, one, two)]

    def split(parts):
        zero = jnp.zeros_like(parts[4])
        return parts[Z] + jnp.where(late, parts[4], zero), parts[1] + parts[2] + parts[3] + jnp.where(late, zero, parts[4])

    class Head:
        pass

    heads = []
    for head in range(HEADS):
        x = Head()
        load_keys(me, kv_refs, keys.at[head], vals.at[head], head)
        lanes = slice(WIDE * head, WIDE * (head + 1))
        q_tile = q_ref[Z, :, lanes]
        x.q = choose(spread_heads(q_tile[:HALF]), spread_heads(q_tile[HALF:]))
        x.scores, x.tops, x.exps, x.sums, x.outs = [], [], [], [], []
        heads.append(x)

    def score(head, i):
        x = heads[head]
        start, block, masked, which = plan[i]
        s = nt(keys[head, pl.ds(start, CHUNK), :], x.q[which])
        if masked:
            s = jnp.where(gap <= block * HALF - start, s, NEG_BIG)
        x.scores.append(s)
        x.tops.append(jnp.max(s, axis=Z, keepdims=True))

    def top(head):
        x = heads[head]
        t = x.tops
        top_b = jnp.maximum(jnp.maximum(t[1], t[2]), t[3])
        top_a = jnp.where(late, jnp.maximum(t[Z], t[4]), t[Z]) * scale2
        top_b = jnp.where(late, top_b, jnp.maximum(top_b, t[4])) * scale2
        x.top = choose(top_a, top_b)

    def expo(head, i):
        x = heads[head]
        e = jnp.exp2(x.scores[i] * scale2 - x.top[plan[i][3]])
        x.exps.append(e if NORM else e.astype(BF))
        x.sums.append(jnp.sum(e, axis=Z, keepdims=True))

    def total(head):
        x = heads[head]
        sum_a, sum_b = split(x.sums)
        lse_ref[head, Z:1, :] = x.top[Z] + jnp.log2(sum_a)
        lse_ref[head, 1:2, :] = x.top[1] + jnp.log2(sum_b)
        x.inv = choose(1.0 / sum_a, 1.0 / sum_b)

    def value(head, i):
        x = heads[head]
        p = (x.exps[i] * x.inv[plan[i][3]]).astype(BF) if NORM else x.exps[i]
        x.outs.append(tn(vals[head, pl.ds(plan[i][Z], CHUNK), :], p))

    def finish(head):
        x = heads[head]
        out_a, out_b = split(x.outs)
        if not NORM:
            out_a, out_b = out_a * x.inv[Z], out_b * x.inv[1]
        gather_heads(out_a, o_ref, Z, WIDE * head)
        gather_heads(out_b, o_ref, HALF, WIDE * head)

    n = len(plan)
    for head in range(HEADS + 2):
        for i in range(n):
            if head < HEADS:
                score(head, i)
            if Z <= head - 1 < HEADS:
                if i == Z:
                    top(head - 1)
                expo(head - 1, i)
            if Z <= head - 2 < HEADS:
                if i == Z:
                    total(head - 2)
                value(head - 2, i)
        if Z <= head - 2 < HEADS:
            finish(head - 2)


def bwd_kernel(scale, scale2, aliased, me_ref, q_ref, g_ref, lse_ref, *refs):
    kv_refs = refs[:8]
    refs = refs[8 + (1 if aliased else Z):]
    dq_ref, keep_ref, send_ref, keys, vals, grads = refs
    me = me_ref[Z]
    gap = lag()
    late, plan = tile_plan(me)
    low = low_lanes(CHUNK)

    def choose(one, two):
        return [one, two, jnp.where(late, one, two)]

    def split(parts):
        zero = jnp.zeros_like(parts[4])
        return parts[Z] + jnp.where(late, parts[4], zero), parts[1] + parts[2] + parts[3] + jnp.where(late, zero, parts[4])

    class Head:
        pass

    heads = []
    for head in range(HEADS):
        x = Head()
        load_keys(me, kv_refs, keys.at[head], vals.at[head], head)
        lanes = slice(WIDE * head, WIDE * (head + 1))
        q_tile, g_tile = q_ref[Z, :, lanes], g_ref[Z, :, lanes]
        x.q = choose(spread_heads(q_tile[:HALF]), spread_heads(q_tile[HALF:]))
        x.g = choose(spread_heads(g_tile[:HALF]), spread_heads(g_tile[HALF:]))
        x.lse = choose(lse_ref[head, Z:1, :], lse_ref[head, 1:2, :])
        x.probs, x.dprobs, x.deltas, x.dqs, x.dks, x.dvs = [], [], [], [], [], []
        heads.append(x)

    def prob(head, i):
        x = heads[head]
        start, block, masked, which = plan[i]
        s = nt(keys[head, pl.ds(start, CHUNK), :], x.q[which])
        if masked:
            s = jnp.where(gap <= block * HALF - start, s, NEG_BIG)
        p = jnp.exp2(s * scale2 - x.lse[which])
        dp = nt(vals[head, pl.ds(start, CHUNK), :], x.g[which]).astype(BF)
        x.probs.append(p)
        x.dprobs.append(dp)
        x.deltas.append(jnp.sum(p * dp.astype(F32), axis=Z, keepdims=True))

    def delta(head):
        x = heads[head]
        x.delta = choose(*split(x.deltas))

    def grad(head, i):
        x = heads[head]
        start, _, _, which = plan[i]
        p, dp = x.probs[i], x.dprobs[i]
        ds = (p * (dp.astype(F32) - x.delta[which])).astype(BF)
        x.dvs.append(nn(p.astype(BF), x.g[which]))
        x.dks.append(nn(ds, x.q[which]))
        x.dqs.append(tn(keys[head, pl.ds(start, CHUNK), :], ds))

    def finish(head):
        x = heads[head]
        dq_a, dq_b = split(x.dqs)
        gather_heads(dq_a * scale, dq_ref, Z, WIDE * head)
        gather_heads(dq_b * scale, dq_ref, HALF, WIDE * head)
        zero = jnp.zeros_like(x.dks[4])

        def by_chunk(parts):
            return [parts[Z] + parts[1], parts[2] + jnp.where(late, parts[4], zero), parts[3],
                    jnp.where(late, zero, parts[4])]

        for chunk, (dk, dv) in enumerate(zip(by_chunk(x.dks), by_chunk(x.dvs))):
            dk = (dk + pltpu.roll(dk, HALF, 1)) * scale
            dv = dv + pltpu.roll(dv, HALF, 1)
            both = jnp.where(low, dk, dv)
            for sub in range(4):
                block = 4 * chunk + sub
                dev, base = (block, Z) if block < 8 else (15 - block, HALF)
                grads[dev ^ me, base:base + HALF, LANES * head:LANES * (head + 1)] = both[sub * HALF:(sub + 1) * HALF]

    n = len(plan)
    for head in range(HEADS + 1):
        for i in range(n):
            if head < HEADS:
                prob(head, i)
            if head >= 1:
                if i == Z:
                    delta(head - 1)
                grad(head - 1, i)
        if head >= 1:
            finish(head - 1)
    for one in range(2):
        for two in range(2):
            slot = jnp.where(pl.program_id(1) == Z, 2 * two + one, 2 * one + two)
            keep_ref[Z, one, two, Z] = grads[2 * slot]
            send_ref[Z, one, two, Z] = grads[2 * slot + 1]


def attn_fwd(me, q, kvs, first, total, o_prev=None):
    count = kvs[Z].shape[Z]
    scale2 = 0.125 * math.log2(math.e)
    aliased = o_prev is not None
    row = lambda b, g, m: (first + b, Z, g)
    kv_spec = pl.BlockSpec((1, LANES, LANES * HEADS), lambda b, g, m: (b, Z, g))
    grid_spec = pltpu.PrefetchScalarGridSpec(
        num_scalar_prefetch=1, grid=(count, 4 // HEADS),
        in_specs=[pl.BlockSpec((1, LANES, WIDE * HEADS), row)] + [kv_spec] * 8 + ([pl.BlockSpec(memory_space=pl.ANY)] if aliased else []),
        out_specs=[pl.BlockSpec((1, LANES, WIDE * HEADS), row), pl.BlockSpec((HEADS, 2, WIDE), lambda b, g, m: (b * (4 // HEADS) + g, Z, Z))],
        scratch_shapes=[pltpu.VMEM((HEADS, SEQ, LANES), BF), pltpu.VMEM((HEADS, SEQ, LANES), BF)])
    return pl.pallas_call(
        functools.partial(fwd_kernel, scale2, aliased), grid_spec=grid_spec, name='attn_fwd',
        out_shape=[jax.ShapeDtypeStruct((total, LANES, MODEL), BF), jax.ShapeDtypeStruct((count * 4, 2, WIDE), F32)],
        input_output_aliases={10: Z} if aliased else {},
        cost_estimate=timed(6 * count),
        compiler_params=ALL_VMEM,
    )(me, q, *kvs, *([o_prev] if aliased else []))


def attn_bwd(me, q, g, lse, kvs, first, sub, count, dq_prev=None):
    total = q.shape[Z]
    scale = 0.125
    scale2 = scale * math.log2(math.e)
    aliased = dq_prev is not None
    row = lambda b, h, m: (first + b, Z, h)
    kv_spec = pl.BlockSpec((1, LANES, LANES * HEADS), lambda b, h, m: (sub + b, Z, h))
    part = pl.BlockSpec((1, 2, 2, 1, LANES, CHUNK), lambda b, h, m: (h, Z, Z, b, Z, Z))
    part_shape = jax.ShapeDtypeStruct((2, 2, 2, count, LANES, CHUNK), F32)
    grid_spec = pltpu.PrefetchScalarGridSpec(
        num_scalar_prefetch=1, grid=(count, 4 // HEADS),
        in_specs=[pl.BlockSpec((1, LANES, WIDE * HEADS), row), pl.BlockSpec((1, LANES, WIDE * HEADS), row),
                  pl.BlockSpec((HEADS, 2, WIDE), lambda b, h, m: ((sub + b) * (4 // HEADS) + h, Z, Z))] + [kv_spec] * 8
        + ([pl.BlockSpec(memory_space=pl.ANY)] if aliased else []),
        out_specs=[pl.BlockSpec((1, LANES, WIDE * HEADS), row), part, part],
        scratch_shapes=[pltpu.VMEM((HEADS, SEQ, LANES), BF), pltpu.VMEM((HEADS, SEQ, LANES), BF), pltpu.VMEM((8, LANES, LANES * HEADS), F32)])
    return pl.pallas_call(
        functools.partial(bwd_kernel, scale, scale2, aliased), grid_spec=grid_spec, name='attn_bwd',
        out_shape=[jax.ShapeDtypeStruct((total, LANES, MODEL), BF)] + [part_shape] * 2,
        input_output_aliases={12: Z} if aliased else {},
        cost_estimate=timed(10 * count),
        compiler_params=ALL_VMEM,
    )(me, q, g, lse, *kvs, *([dq_prev] if aliased else []))


BITS = {'c': 1, 'x': 2, 'y': 4}
ALL_VMEM = pltpu.CompilerParams(vmem_limit_bytes=63 * 2**20)
FF_PARAMS = pltpu.CompilerParams(vmem_limit_bytes=63 * 2**20)
NEXT = {'x': ('y', 'z'), 'y': ('z', 'x'), 'z': ('x', 'y')}


def swap(values, link):
    if link == 'z':
        return lax.ppermute(values, 'dp', [(Z, 1), (1, Z)])
    return lax.ppermute(values, 'cp', [(i, i ^ BITS[link]) for i in range(8)])


def pick(values, axis, index):
    return lax.index_in_dim(values, index, axis, keepdims=False)


def timed(micros):
    return pl.CostEstimate(flops=int(micros * 9e8), bytes_accessed=1 << 20, transcendentals=Z)


def mm_kernel(product, added, x_ref, w_ref, *refs):
    total = product(x_ref[...], w_ref[...])
    if added:
        total = total + refs[Z][...].astype(F32)
    refs[-1][...] = total.astype(refs[-1].dtype)


def mm(x, w, rows, first, count, width, flip=True, added=None, dtype=BF):
    total, depth = x.shape
    tile = pl.BlockSpec((rows, width), lambda n, t: (t, n))
    w_spec = pl.BlockSpec((width, depth), lambda n, t: (first + n, Z)) if flip else pl.BlockSpec(
        (depth, width), lambda n, t: (Z, first + n))
    return pl.pallas_call(
        functools.partial(mm_kernel, nt if flip else nn, added is not None), grid=(count, total // rows), name='mm',
        in_specs=[pl.BlockSpec((rows, depth), lambda n, t: (t, Z)), w_spec] + ([tile] if added is not None else []),
        out_specs=tile, out_shape=jax.ShapeDtypeStruct((total, count * width), dtype),
        cost_estimate=timed(total * count * width * depth * 2 / 9e8),
        compiler_params=ALL_VMEM)(x, w, *([added] if added is not None else []))


def join_kv(k_ref, v_ref, both):
    @pl.when(pl.program_id(Z) == Z)
    def _():
        for head in range(4):
            both[LANES * head:LANES * head + HALF, :] = k_ref[HALF * head:HALF * head + HALF, :]
            both[LANES * head + HALF:LANES * head + LANES, :] = v_ref[HALF * head:HALF * head + HALF, :]


def kv_kernel(x_ref, k_ref, v_ref, low_ref, high_ref, both):
    join_kv(k_ref, v_ref, both)
    value = nt(x_ref[...], both[...]).astype(BF)
    for index, ref in enumerate((low_ref, high_ref)):
        @pl.when(pl.program_id(Z) // 2 == index)
        def _():
            ref[...] = value


def kv_call(x, w_k, w_v):
    rows, (total, depth) = WIDE, x.shape
    whole = pl.BlockSpec((CHUNK, depth), lambda t: (Z, Z), pipeline_mode=pl.Buffered(1))
    return pl.pallas_call(
        kv_kernel, grid=(total // rows,), name='kv',
        in_specs=[pl.BlockSpec((rows, depth), lambda t: (t, Z)), whole, whole],
        out_specs=[pl.BlockSpec((rows, WIDE), lambda t: (jnp.minimum(t, 1), Z)), pl.BlockSpec((rows, WIDE), lambda t: (jnp.maximum(t - 2, Z), Z))],
        out_shape=[jax.ShapeDtypeStruct((total // 2, WIDE), BF)] * 2,
        scratch_shapes=[pltpu.VMEM((WIDE, depth), BF)], cost_estimate=timed(9), compiler_params=ALL_VMEM)(x, w_k, w_v)


def gx_kernel(h_ref, q_ref, g_ref, w_ref, k_ref, v_ref, *refs):
    out_ref, both = refs[-2:]
    join_kv(k_ref, v_ref, both)
    total = nn(q_ref[...], w_ref[...]) + nn(g_ref[...], both[...])
    out_ref[...] = (h_ref[...].astype(F32) + total).astype(BF)


def gx_call(grad_h, grad_q, grad_kv, w_q, w_k, w_v, half, prev=None):
    rows, (total, depth) = WIDE, grad_h.shape
    width = depth // 2
    aliased = prev is not None
    tile = pl.BlockSpec((rows, width), lambda t: (t, half))
    once = lambda count: pl.BlockSpec((count, width), lambda t: (Z, half), pipeline_mode=pl.Buffered(1))
    return pl.pallas_call(
        gx_kernel, grid=(total // rows,), name='gx',
        in_specs=[tile, pl.BlockSpec((rows, depth), lambda t: (t, Z)), pl.BlockSpec((rows, WIDE), lambda t: (t, Z)), once(depth), once(CHUNK),
                  once(CHUNK)] + ([pl.BlockSpec(memory_space=pl.ANY)] if aliased else []),
        out_specs=tile, out_shape=jax.ShapeDtypeStruct((total, depth), BF), scratch_shapes=[pltpu.VMEM((WIDE, width), BF)],
        input_output_aliases={6: Z} if aliased else {}, cost_estimate=timed(14), compiler_params=ALL_VMEM,
    )(grad_h, grad_q, grad_kv, w_q, w_k, w_v, *([prev] if aliased else []))


def ff_kernel(bits_ref, h_ref, w_ref, ga_ref, at_ref, gu_ref, held, turned):
    root = math.sqrt(2.0 / math.pi)
    width = w_ref.shape[1]
    for lo in range(Z, width, CHUNK):
        cut = slice(lo, min(lo + CHUNK, width))
        u = held[:, cut]
        held[:, cut] = nn(h_ref[...], w_ref[:, cut])
        rise = (root * 0.044715) * (u * u)
        t = jnp.tanh(u * (root + rise))
        up, down, half_u = 1.0 + t, 1.0 - t, 0.5 * u
        slope = up * (0.5 + (half_u * down) * (root + 3.0 * rise))
        gu_ref[:, cut] = (ga_ref[:, cut].astype(F32) * slope).astype(BF)
        turned[cut, :] = (half_u * up).T.astype(BF)
    for x in range(2):
        for c in range(2):
            lo = (2 * x + c) * FF_ROWS
            at_ref[Z, Z, x ^ bits_ref[2], c ^ bits_ref[3]] = turned[lo:lo + FF_ROWS, :]


def ff_block(bits, h, w_up, ga):
    tokens, width, rows = MODEL, FF_TILE, WIDE
    per = tokens // rows
    steps = 4 * per
    now = lambda i: jnp.minimum(i, steps - 1)
    then = lambda i: jnp.maximum(i - 1, Z)
    grid_spec = pltpu.PrefetchScalarGridSpec(
        num_scalar_prefetch=1, grid=(steps + 1,),
        in_specs=[pl.BlockSpec((rows, MODEL), lambda i, m: (now(i) % per, Z)),
                  pl.BlockSpec((MODEL, width), lambda i, m: (Z, now(i) // per)),
                  pl.BlockSpec((rows, width), lambda i, m: (then(i) % per, then(i) // per))],
        out_specs=[pl.BlockSpec((1, 1, 2, 2, FF_ROWS, rows), lambda i, m: ((then(i) // per // 2) ^ m[Z], (then(i) // per % 2) ^ m[1], Z, Z, Z, then(i) % per)),
                   pl.BlockSpec((rows, width), lambda i, m: (then(i) % per, then(i) // per))],
        scratch_shapes=[pltpu.VMEM((rows, width), F32), pltpu.VMEM((width, rows), BF)])
    return pl.pallas_call(
        ff_kernel, grid_spec=grid_spec, name='ff_block',
        out_shape=[jax.ShapeDtypeStruct((2, 2, 2, 2, FF_ROWS, tokens), BF), jax.ShapeDtypeStruct((tokens, 5632), BF)],
        cost_estimate=timed(60), compiler_params=FF_PARAMS)(bits, h, w_up, ga)


def color_of(n, plan):
    edge, color = Z, Z
    for _, count in plan[:-1]:
        edge += count
        color = color + (n >= edge).astype(jnp.int32)
    return color


def pair_kernel(plan, rows, turned, *refs):
    n, steps = pl.program_id(Z), sum(count for _, count in plan)
    count = len(plan)
    if turned:
        left, refs = refs[Z], refs[1:]
    else:
        source, refs, (parts, left, load_sem) = refs[Z], refs[1:-3], refs[-3:]
    me = lax.axis_index('cp')
    bits = (lax.axis_index('dp'), me // 4, (me // 2) % 2, me % 2)

    def load(place, core):
        flips = (place // 4, place // 2 % 2, place % 2, core)
        block = sum((1 - bit if flip else bit) * weight for bit, flip, weight in zip(bits, flips, (8, 4, 2, 1)))
        columns = pl.ds(pl.multiple_of(block * LANES, LANES), LANES)
        return pltpu.make_async_copy(source.at[:, columns], parts.at[place, core], load_sem.at[place, core])

    right, outs = refs[Z], refs[1:1 + 2 * count]
    mine, sent, came, send_sem, recv_sem, free_sem = refs[1 + 2 * count:]
    other = {'cp': me + 1 - 2 * (me % 2)}
    mesh_id = pl.DeviceIdType.MESH
    now, then = n % 2, (n + 1) % 2

    def copy(slot):
        return pltpu.make_async_remote_copy(src_ref=sent.at[slot], dst_ref=came.at[slot], send_sem=send_sem.at[slot],
                                            recv_sem=recv_sem.at[slot], device_id=other, device_id_type=mesh_id)

    @pl.when(n == Z)
    def _():
        for core in () if turned else (1, Z):
            for place in range(8):
                load(place, core).start()
        barrier = pltpu.get_barrier_semaphore()
        pl.semaphore_signal(barrier, inc=1, device_id=other, device_id_type=mesh_id)
        pl.semaphore_wait(barrier, 1)

    @pl.when(n >= 3)
    def _():
        pl.semaphore_wait(free_sem, 1)

    @pl.when(n >= 1)
    def _():
        copy(then).start()

    def products(first):
        some = 1 if turned else 4
        for core, dest in ((1, sent), (Z, mine)):
            for place in range(Z, 8, some):
                group = range(place, place + some)
                for k in group if first else ():
                    load(k, core).wait()
                    left[k, core] = parts[k, core].T
                tile = jnp.concatenate([left[k, core] for k in group], axis=Z)
                dest[now, place:place + some] = nn(tile, right[...]).reshape(some, rows, -1)

    if not turned:
        @pl.when(n == Z)
        def _():
            products(True)

    @pl.when((n >= (Z if turned else 1)) & (n < steps))
    def _():
        products(False)

    @pl.when(n >= 1)
    def _():
        copy(then).wait()
        color = color_of(n - 1, plan)
        for index, (split, _) in enumerate(plan):
            @pl.when(color == index)
            def _():
                for place in range(8):
                    z, y, x = place // 4, place // 2 % 2, place % 2
                    half, k = {'z': (z, 2 * y + x), 'y': (y, 2 * z + x), 'x': (x, 2 * z + y)}[split]
                    outs[2 * index + 1 - half][k] = mine[then, place] + came[then, place]

    @pl.when((n >= 1) & (n < steps - 1))
    def _():
        pl.semaphore_signal(free_sem, inc=1, device_id=other, device_id_type=mesh_id)


def pair_call(left, right, plan, tile, call_id):
    turned = left.ndim == 4
    rows = left.shape[2] if turned else LANES
    steps = sum(count for _, count in plan)
    out_specs, out_shape, edge = [], [], Z
    for _, count in plan:
        spec = pl.BlockSpec((4, rows, tile), lambda n, edge=edge, count=count: (Z, Z, jnp.clip(n - 1 - edge, Z, count - 1)))
        out_specs += [spec, spec]
        out_shape += [jax.ShapeDtypeStruct((4, rows, count * tile), F32)] * 2
        edge += count
    both = pltpu.VMEM((2, 8, rows, tile), F32)
    two = pltpu.SemaphoreType.DMA((2,))
    staging = [] if turned else [pltpu.VMEM((8, 2, MODEL, LANES), BF), pltpu.VMEM((8, 2, rows, MODEL), BF), pltpu.SemaphoreType.DMA((8, 2))]
    whole = pl.BlockSpec((8, 2, rows, MODEL), lambda n: (Z, Z, Z, Z), pipeline_mode=pl.Buffered(1))
    return pl.pallas_call(
        functools.partial(pair_kernel, plan, rows, turned), grid=(steps + 1,), name='pair',
        in_specs=[whole if turned else pl.BlockSpec(memory_space=pl.ANY),
                  pl.BlockSpec((MODEL, tile), lambda n: (Z, jnp.minimum(n, steps - 1)))],
        out_specs=out_specs, out_shape=out_shape,
        scratch_shapes=[both, both, both, two, two, pltpu.SemaphoreType.REGULAR, *staging],
        cost_estimate=timed(16 * rows * steps * tile * 4096 / 9e8),
        compiler_params=pltpu.CompilerParams(vmem_limit_bytes=63 * 2**20, collective_id=call_id, has_side_effects=True),
    )(left, right)


def halve(keep, got, axis):
    return tuple(pick(keep, axis, k) + pick(got, axis, k) for k in (1, Z))


def weight_grad(left, right, plan, tile, call_id, flip=False):
    outs = pair_call(left, right, plan, tile, call_id)
    keeps, gots, fars = [], [], []
    for (split, _), send, keep in zip(plan, outs[::2], outs[1::2]):
        shape = (2, 2, *keep.shape[1:])
        got = swap(send, split).reshape(shape)
        send, keep = lax.optimization_barrier(halve(keep.reshape(shape), got, Z if split == 'y' else 1))
        got = swap(send, NEXT[split][Z])
        keeps.append(keep)
        gots.append(got)
        fars.append(swap(keep[1] + got[1], NEXT[split][1]))
    return final(keeps, gots, fars, flip)


def final_kernel(flip, *refs):
    count, edge = len(refs) // 3, Z
    for index in range(count):
        keep, got, far = refs[index:-1:count]
        total = (keep[Z] + got[Z] + far[...]) / 16
        cut = slice(edge, edge + total.shape[1])
        edge = cut.stop
        if flip:
            refs[-1][cut, :] = total.T
        else:
            refs[-1][:, cut] = total


def final(keeps, gots, fars, flip):
    shape = (fars[Z].shape[Z], sum(far.shape[1] for far in fars))
    shape = shape[::-1] if flip else shape
    two = [pl.BlockSpec((1, *far.shape), lambda n: (Z, Z, Z)) for far in fars]
    one = [pl.BlockSpec(far.shape, lambda n: (Z, Z)) for far in fars]
    return pl.pallas_call(
        functools.partial(final_kernel, flip), grid=(1,), name='final', in_specs=two + two + one,
        out_specs=pl.BlockSpec(shape, lambda n: (Z, Z)), out_shape=jax.ShapeDtypeStruct(shape, F32),
        cost_estimate=timed(4), compiler_params=ALL_VMEM)(*keeps, *gots, *fars)


def small_kernel(bits_ref, *refs):
    right = refs[2][...]
    for core in range(2):
        refs[3 + core][Z] = tn(refs[core][...], right)


def small_grad(bits, left, right):
    def column(core):
        return lambda k, m: (Z, ((k % 2) ^ m[Z]) * 8 + ((k // 4) ^ m[1]) * 4 + ((k // 2 % 2) ^ m[2]) * 2 + (core ^ m[3]))

    out = pl.BlockSpec((1, LANES, WIDE), lambda k, m: (k, Z, Z))
    grid_spec = pltpu.PrefetchScalarGridSpec(
        num_scalar_prefetch=1, grid=(8,),
        in_specs=[pl.BlockSpec((MODEL, LANES), column(core)) for core in range(2)] + [pl.BlockSpec((MODEL, WIDE), lambda k, m: (Z, Z))],
        out_specs=[out, out])
    keep, send = pl.pallas_call(small_kernel, grid_spec=grid_spec, name='small', out_shape=[jax.ShapeDtypeStruct((8, LANES, WIDE), F32)] * 2,
                                cost_estimate=timed(8), compiler_params=ALL_VMEM)(bits, left, left, right)
    for link in 'cyx':
        got, half = swap(send, link), keep.shape[Z] // 2
        send, keep = lax.optimization_barrier((keep[half:] + got[half:], keep[:half] + got[:half]))
    return (keep[Z] + swap(send, 'z')[Z]) / 16


def join_kernel(*refs):
    row = Z
    for chunk in range(Z, len(refs) - 1, 4):
        rows = slice(row, row + refs[chunk].shape[Z])
        row = rows.stop
        for color in range(2):
            total, far = refs[chunk + 2 * color:chunk + 2 * color + 2]
            refs[-1][rows, :, CHUNK * color:CHUNK * (color + 1)] = (total[...] + far[...]).astype(BF)


def join(parts):
    return pl.pallas_call(join_kernel, name='join', out_shape=jax.ShapeDtypeStruct((16, LANES, WIDE), BF),
                          cost_estimate=timed(4), compiler_params=ALL_VMEM)(*parts)


def gather_kv(kv, order):
    held = {Z: kv}
    for link in order:
        held.update({pos ^ BITS[link]: swap(tile, link) for pos, tile in list(held.items())})
    return [held[pos] for pos in range(8)]


def reduce_dkv(keep, send):
    got = swap(send, 'c')
    parts = []
    for color, (first, second) in enumerate((('x', 'y'), ('y', 'x'))):
        more = swap(keep[color, 1] + got[color, 1], first)
        send, total = lax.optimization_barrier(tuple(keep[color, Z, k] + got[color, Z, k] + more[k] for k in (1, Z)))
        parts += [total, swap(send, second)]
    return parts


CHUNKS = ((Z, 8), (8, 4), (12, 4))
PLAN_UP = (('z', 5), ('y', 3), ('x', 3))
PLAN_D = (('z', 3), ('y', 3), ('x', 2))


def solution(mesh):
    def per_device(x_loc, cot_loc, w_q, w_k, w_v, w_o, w_up, w_down):
        batch, seq, d_model = x_loc.shape
        tokens = batch * seq
        me = lax.axis_index('cp').astype(jnp.int32)
        me_one = me.reshape(1)
        bits = jnp.stack([lax.axis_index('dp').astype(jnp.int32), me >> 2, (me >> 1) & 1, me & 1])
        x2, cot2 = x_loc.reshape(tokens, d_model), cot_loc.reshape(tokens, d_model)
        w_q2, w_k2, w_v2, w_o2 = (w.transpose(1, 2, Z).reshape(-1, d_model) for w in (w_q, w_k, w_v, w_o))

        kvs = [kv.reshape(batch // 2, seq, -1) for kv in kv_call(x2, w_k2, w_v2)]
        gathered = [gather_kv(kvs[Z], 'xyc'), gather_kv(kvs[1], 'yxc')]
        q = mm(x2, w_q2, WIDE, Z, 2, SEQ).reshape(batch, seq, -1)
        grad_act = mm(cot2, w_down, WIDE, Z, 4, FF_TILE)

        o, lse_first = attn_fwd(me_one, q, gathered[Z], Z, batch)
        o, lse_second = attn_fwd(me_one, q, gathered[1], batch // 2, batch, o)
        lse = [lse_first, lse_second]
        o2 = o.reshape(tokens, -1)
        h = mm(o2, w_o2, WIDE, Z, 2, SEQ, False, x2)

        act_t, grad_u = ff_block(bits, h, w_up, grad_act)
        grad_w_up = weight_grad(h, grad_u, PLAN_UP, WIDE, Z)
        grad_w_down = weight_grad(act_t.reshape(8, 2, -1, tokens), cot2, PLAN_D, CHUNK, 1)
        grad_h = mm(grad_u, w_up, WIDE, Z, 4, WIDE, True, cot2)
        grad_o = mm(grad_h, w_o2, WIDE, Z, 2, SEQ).reshape(batch, seq, -1)

        grad_q, grad_kv = None, []
        for part, (first, count) in enumerate(CHUNKS):
            side, sub = first // 8, first % 8
            grad_q, keep, send = attn_bwd(me_one, q, grad_o, lse[side], gathered[side], first, sub, count, grad_q)
            grad_kv += reduce_dkv(keep, send)
            if part == Z:
                grad_w_o = weight_grad(grad_h, o2, PLAN_D, CHUNK, 2, True)
        grad_q2 = grad_q.reshape(tokens, -1)
        grad_w_q = weight_grad(x2, grad_q2, PLAN_D, CHUNK, 3, True)
        grad_kv2 = join(grad_kv).reshape(tokens, -1)
        grad_w_kv = small_grad(bits, x2, grad_kv2).reshape(-1, 4, 2, HALF)
        grad_x = None
        for part in range(2):
            grad_x = gx_call(grad_h, grad_q2, grad_kv2, w_q2, w_k2, w_v2, part, grad_x)
        return (grad_x.reshape(x_loc.shape), grad_w_q.reshape(32, HALF, -1).transpose(2, Z, 1), grad_w_kv[:, :, Z], grad_w_kv[:, :, 1],
                grad_w_o.reshape(32, HALF, -1).transpose(2, Z, 1), grad_w_up, grad_w_down)

    act_spec = P('dp', 'cp', None)
    rep_three, rep_two = P(None, None, None), P(None, None)
    grad_three, grad_two = P(('dp', 'cp'), None, None), P(('dp', 'cp'), None)
    return jax.shard_map(per_device, mesh=mesh,
                         in_specs=(act_spec, act_spec, rep_three, rep_three, rep_three, rep_three, rep_two, rep_two),
                         out_specs=(act_spec, grad_three, grad_three, grad_three, grad_three, grad_two, grad_two),
                         check_vma=False)
```
